8 devices in a mesh: dp: 8 (over z, y, x, core).
Axes of the slice: x: 2, y: 2, z: 1, core: 2. Of those that a mesh axis runs over, the one named last changes fastest.
Arguments:
- feats: bfloat16 [4096, 768], P('dp')
- frontier: int32 [262144], P('dp')
- nbr_l1: int32 [65536, 15], P('dp')
- mask_l1: int32 [65536, 15], P('dp')
- nbr_l2: int32 [16384, 10], P('dp')
- mask_l2: int32 [16384, 10], P('dp')
- nbr_l3: int32 [4096, 5], P('dp')
- mask_l3: int32 [4096, 5], P('dp')
- labels: int32 [4096], P('dp')
- seed_mask: int32 [4096], P('dp')
- params: float32 [604313], replicated
- adam_m: float32 [604313], replicated
- adam_v: float32 [604313], replicated
Outputs:
- output 1: float32 [], replicated
- output 2: float32 [604313], replicated
- output 3: float32 [604313], replicated
- output 4: float32 [604313], replicated
All inputs are finite; a program needn't handle non-finite values.
Results may differ from the reference program's by a relative error of at most 0.00173952.
Values are sent between devices in bfloat16 or wider.
A program may use at most 1 GiB of HBM per device.

```python
import jax
import jax.numpy as jnp
from jax import lax

DP = 8
NODES_DEV = 512
SEEDS = 512
FEAT = 768
CLASSES = 153
HIDDEN = 256
STEP = 10

N_ZERO = 64 * SEEDS
N_ONE = 16 * SEEDS
N_TWO = 4 * SEEDS
HUB_OWNERS = DP // 8
UNIF_PER = (3 * N_ZERO) // (4 * DP)
HUB_PER = N_ZERO // (4 * HUB_OWNERS)
HOT_ROWS = min(256, NODES_DEV)
LN_EPS = 1e-5
BETA_ONE = 0.9
BETA_TWO = 0.999
ADAM_LR = 3e-3
ADAM_EPS = 1e-8


def param_shapes(feat, classes):
    return [(feat, HIDDEN), (feat, HIDDEN), (HIDDEN,), (HIDDEN,), (HIDDEN,),
            (HIDDEN, HIDDEN), (HIDDEN, HIDDEN), (HIDDEN,), (HIDDEN,), (HIDDEN,),
            (HIDDEN, classes), (HIDDEN, classes), (classes,)]


def unpack(flat, feat, classes):
    pieces = []
    offset = 0
    for pshape in param_shapes(feat, classes):
        count_el = 1
        for extent in pshape:
            count_el = count_el * extent
        pieces.append(flat[offset:offset + count_el].reshape(pshape))
        offset = offset + count_el
    return pieces


def draw_structure(key):
    keys = jax.random.split(key, 12)
    hub_list = jax.random.permutation(keys[0], DP)[:HUB_OWNERS].astype(jnp.int32)
    owner_list = jnp.concatenate([jnp.repeat(jnp.arange(DP, dtype=jnp.int32), UNIF_PER),
                                  jnp.repeat(hub_list, HUB_PER, total_repeat_length=HUB_OWNERS * HUB_PER)])
    hub_flag = jnp.concatenate([jnp.zeros((DP * UNIF_PER,), jnp.int32), jnp.ones((HUB_OWNERS * HUB_PER,), jnp.int32)])
    slot_perm = jax.vmap(lambda sub: jax.random.permutation(sub, N_ZERO))(jax.random.split(keys[1], DP))
    owners = owner_list[slot_perm]
    is_hub = hub_flag[slot_perm]
    any_rows = jax.random.randint(keys[2], (DP, N_ZERO), 0, NODES_DEV)
    hot_rows = jax.random.randint(keys[3], (DP, N_ZERO), 0, HOT_ROWS)
    row_pick = jnp.where(is_hub == 1, hot_rows, any_rows)
    frontier = (owners * NODES_DEV + row_pick).reshape(-1).astype(jnp.int32)
    nbr_l1 = jax.random.randint(keys[4], (DP * N_ONE, 15), 0, N_ZERO)
    mask_l1 = (jax.random.randint(keys[5], (DP * N_ONE, 15), 0, 4) > 0).astype(jnp.int32)
    nbr_l2 = jax.random.randint(keys[6], (DP * N_TWO, 10), 0, N_ONE)
    mask_l2 = (jax.random.randint(keys[7], (DP * N_TWO, 10), 0, 4) > 0).astype(jnp.int32)
    nbr_l3 = jax.random.randint(keys[8], (DP * SEEDS, 5), 0, N_TWO)
    mask_l3 = (jax.random.randint(keys[9], (DP * SEEDS, 5), 0, 4) > 0).astype(jnp.int32)
    valid = jax.random.randint(keys[10], (DP, SEEDS), 0, 8) > 0
    seed_mask = jnp.where(jnp.arange(SEEDS)[None, :] == 0, True, valid).astype(jnp.int32).reshape(-1)
    labels = jax.random.randint(keys[11], (DP * SEEDS,), 0, CLASSES)
    return frontier, nbr_l1, mask_l1, nbr_l2, mask_l2, nbr_l3, mask_l3, labels, seed_mask


def setup_inputs(seed: int = 0) -> dict:
    key = jax.random.key(seed)
    key_struct, key_vals = jax.random.split(key)
    frontier, nbr_l1, mask_l1, nbr_l2, mask_l2, nbr_l3, mask_l3, labels, seed_mask = draw_structure(key_struct)
    vkeys = jax.random.split(key_vals, 4)
    feats = jax.random.normal(vkeys[0], (DP * NODES_DEV, FEAT), jnp.float32).astype(jnp.bfloat16)
    pieces = []
    for index, pshape in enumerate(param_shapes(FEAT, CLASSES)):
        noise = jax.random.normal(jax.random.fold_in(vkeys[1], index), pshape, jnp.float32)
        if len(pshape) == 2:
            piece = noise * pshape[0] ** -0.5
        elif index in (3, 8):
            piece = 1.0 + 0.3 * noise
        else:
            piece = 0.3 * noise
        pieces.append(piece.reshape(-1))
    params = jnp.concatenate(pieces)
    grad_scale = 0.1 * (DP * SEEDS) ** -0.5
    adam_m = grad_scale * jax.random.normal(vkeys[2], params.shape, jnp.float32)
    adam_v = (grad_scale * jax.random.uniform(vkeys[3], params.shape, jnp.float32, 0.5, 1.5)) ** 2
    return {'feats': feats, 'frontier': frontier, 'nbr_l1': nbr_l1, 'mask_l1': mask_l1,
            'nbr_l2': nbr_l2, 'mask_l2': mask_l2, 'nbr_l3': nbr_l3, 'mask_l3': mask_l3,
            'labels': labels, 'seed_mask': seed_mask, 'params': params,
            'adam_m': adam_m, 'adam_v': adam_v}


def layer_post(z, gain, shift):
    act = jax.nn.relu(z)
    mean_act = jnp.mean(act, axis=-1, keepdims=True)
    centred = act - mean_act
    var_act = jnp.mean(centred * centred, axis=-1, keepdims=True)
    return centred * lax.rsqrt(var_act + LN_EPS) * gain + shift


def neighbor_mean(table, nbr_idx, nbr_mask):
    gathered = jnp.take(table, nbr_idx, axis=0).astype(jnp.float32)
    weight = nbr_mask.astype(jnp.float32)
    summed = jnp.einsum('nk,nkd->nd', weight, gathered)
    count = jnp.maximum(jnp.sum(weight, axis=-1), 1.0)
    return summed / count[:, None]


def dense_pair(self_rows, agg_rows, w_self, w_nbr, bias):
    return (jnp.dot(self_rows, w_self.astype(jnp.bfloat16), preferred_element_type=jnp.float32)
            + jnp.dot(agg_rows, w_nbr.astype(jnp.bfloat16), preferred_element_type=jnp.float32) + bias)


def device_ce(flat, frontier_dev, nbr_l1, mask_l1, nbr_l2, mask_l2, nbr_l3, mask_l3, labels, seed_mask, feats):
    pieces = unpack(flat, FEAT, CLASSES)
    h_zero = jnp.take(feats, frontier_dev, axis=0)
    agg_one = neighbor_mean(h_zero, nbr_l1, mask_l1).astype(jnp.bfloat16)
    z_one = dense_pair(h_zero[:N_ONE], agg_one, pieces[0], pieces[1], pieces[2])
    h_one = layer_post(z_one, pieces[3], pieces[4]).astype(jnp.bfloat16)
    agg_two = neighbor_mean(h_one, nbr_l2, mask_l2).astype(jnp.bfloat16)
    z_two = dense_pair(h_one[:N_TWO], agg_two, pieces[5], pieces[6], pieces[7])
    h_two = layer_post(z_two, pieces[8], pieces[9]).astype(jnp.bfloat16)
    agg_three = neighbor_mean(h_two, nbr_l3, mask_l3).astype(jnp.bfloat16)
    logits = dense_pair(h_two[:SEEDS], agg_three, pieces[10], pieces[11], pieces[12])
    log_norm = jax.nn.logsumexp(logits, axis=-1)
    picked = jnp.take_along_axis(logits, labels[:, None], axis=1)[:, 0]
    return jnp.sum((log_norm - picked) * seed_mask.astype(jnp.float32))


def reference(feats, frontier, nbr_l1, mask_l1, nbr_l2, mask_l2, nbr_l3, mask_l3, labels, seed_mask, params, adam_m, adam_v):
    total = jnp.maximum(jnp.sum(seed_mask), 1).astype(jnp.float32)
    per_dev = (frontier.reshape(DP, N_ZERO), nbr_l1.reshape(DP, N_ONE, 15), mask_l1.reshape(DP, N_ONE, 15),
               nbr_l2.reshape(DP, N_TWO, 10), mask_l2.reshape(DP, N_TWO, 10),
               nbr_l3.reshape(DP, SEEDS, 5), mask_l3.reshape(DP, SEEDS, 5),
               labels.reshape(DP, SEEDS), seed_mask.reshape(DP, SEEDS))

    def loss_fn(flat):
        sums = lax.map(lambda batch: device_ce(flat, *batch, feats), per_dev)
        return jnp.sum(sums) / total

    loss, grads = jax.value_and_grad(loss_fn)(params)
    m_new = BETA_ONE * adam_m + (1.0 - BETA_ONE) * grads
    v_new = BETA_TWO * adam_v + (1.0 - BETA_TWO) * grads * grads
    m_hat = m_new / (1.0 - BETA_ONE ** STEP)
    v_hat = v_new / (1.0 - BETA_TWO ** STEP)
    p_new = params - ADAM_LR * m_hat / (jnp.sqrt(v_hat) + ADAM_EPS)
    return loss, p_new, m_new, v_new
```

```python
import functools

import jax
import jax.numpy as jnp
from jax import lax
from jax.experimental import pallas as pl
from jax.experimental.pallas import tpu as pltpu
from jax.sharding import PartitionSpec as P

HIDDEN = 256
STEP = 10
LN_EPS = 1e-5
BETA_ONE = 0.9
BETA_TWO = 0.999
ADAM_LR = 3e-3
ADAM_EPS = 1e-8
F32 = jnp.float32
BF16 = jnp.bfloat16
VMEM_ALL = 60 * 1024 * 1024


def param_shapes(feat, classes):
    return [(feat, HIDDEN), (feat, HIDDEN), (HIDDEN,), (HIDDEN,), (HIDDEN,),
            (HIDDEN, HIDDEN), (HIDDEN, HIDDEN), (HIDDEN,), (HIDDEN,), (HIDDEN,),
            (HIDDEN, classes), (HIDDEN, classes), (classes,)]


def class_count(n_params, feat):
    return (n_params - 2 * feat * HIDDEN - 6 * HIDDEN - 2 * HIDDEN * HIDDEN) // (2 * HIDDEN + 1)


def unpack(flat, feat, classes):
    pieces = []
    offset = 0
    for pshape in param_shapes(feat, classes):
        count_el = 1
        for extent in pshape:
            count_el = count_el * extent
        pieces.append(flat[offset:offset + count_el].reshape(pshape))
        offset = offset + count_el
    return pieces


def params_of(*sem, vmem=VMEM_ALL):
    return pltpu.CompilerParams(dimension_semantics=sem, vmem_limit_bytes=vmem)


def emit_codes(ids, mask, shift, out_ref):
    n = ids.shape[1]
    node = lax.broadcasted_iota(jnp.int32, (16, n), 1)
    lo = (ids & 255).astype(F32)
    code = jnp.where(mask > 0, (ids >> 8) * 16 + (node & 15) - shift, -384).astype(F32)
    count = jnp.maximum(jnp.sum(mask, axis=0, keepdims=True), 1).astype(F32)
    count = jnp.broadcast_to(count, (16, n))
    for c in range(n // 128):
        lanes = slice(c * 128, (c + 1) * 128)
        stack = jnp.concatenate([lo[:, lanes], code[:, lanes], count[:, lanes],
                                 jnp.zeros((80, 128), F32)], axis=0)
        out_ref[lanes, :] = stack.T.astype(BF16)


def pad_rows(x, rows):
    return jnp.concatenate([x, jnp.zeros((rows - x.shape[0], x.shape[1]), x.dtype)], axis=0)


def compose_kernel(front_ref, nbr_ref, mask_ref, out_ref, table_ref):
    n = nbr_ref.shape[1]
    half = front_ref.shape[0] // 2

    @pl.when(pl.program_id(0) == 0)
    def _():
        table_ref[...] = front_ref[0:half, :] + (front_ref[half:2 * half, :] << 12)

    nbr = pad_rows(nbr_ref[...], 16)
    mask = pad_rows(mask_ref[...], 16)
    tiles = [(s, c) for s in range(2) for c in range(n // 128)]
    parts = [nbr[s * 8:s * 8 + 8, c * 128:c * 128 + 128] for s, c in tiles]
    lane = [part & 127 for part in parts]
    row = [part >> 7 for part in parts]
    low = [r & (half - 1) for r in row]

    def step(base, accs):
        accs = list(accs)
        block = table_ref[pl.ds(pl.multiple_of(base * 8, 8), 8), :]
        for u in range(8):
            entry = jnp.broadcast_to(block[u:u + 1, :], (8, 128))
            at = base * 8 + u
            for t in range(len(tiles)):
                got = jnp.take_along_axis(entry, lane[t], axis=1, mode="promise_in_bounds")
                accs[t] = jnp.where(low[t] == at, got, accs[t])
        return tuple(accs)

    accs = lax.fori_loop(0, half // 8, step, tuple(jnp.zeros((8, 128), jnp.int32) for _ in tiles))
    ids = [jnp.where(row[t] >= half, accs[t] >> 12, accs[t]) & 4095 for t in range(len(tiles))]
    cols = n // 128
    ids = jnp.concatenate([jnp.concatenate(ids[s * cols:(s + 1) * cols], axis=1) for s in range(2)], axis=0)
    emit_codes(ids, mask, 0, out_ref)


def codes_kernel(shift, nbr_ref, mask_ref, out_ref):
    emit_codes(pad_rows(nbr_ref[...], 16), pad_rows(mask_ref[...], 16), shift, out_ref)


def compose(frontier, nbr_t, mask_t, block=512):
    n = nbr_t.shape[1]
    rows = frontier.shape[0] // 128
    return pl.pallas_call(
        compose_kernel,
        grid=(n // block,),
        in_specs=[pl.BlockSpec((rows, 128), lambda i: (0, 0)),
                  pl.BlockSpec((nbr_t.shape[0], block), lambda i: (0, i)),
                  pl.BlockSpec((nbr_t.shape[0], block), lambda i: (0, i))],
        out_specs=pl.BlockSpec((block, 128), lambda i: (i, 0)),
        out_shape=jax.ShapeDtypeStruct((n, 128), BF16),
        scratch_shapes=[pltpu.VMEM((rows // 2, 128), jnp.int32)],
        compiler_params=params_of("arbitrary"),
        cost_estimate=pl.CostEstimate(flops=10**9, bytes_accessed=10**7, transcendentals=0),
        name="compose_ids",
    )(frontier.reshape(rows, 128), nbr_t, mask_t)


def codes(nbr_t, mask_t, shift, block=512):
    n = nbr_t.shape[1]
    return pl.pallas_call(
        functools.partial(codes_kernel, shift),
        grid=(n // block,),
        in_specs=[pl.BlockSpec((nbr_t.shape[0], block), lambda i: (0, i)),
                  pl.BlockSpec((nbr_t.shape[0], block), lambda i: (0, i))],
        out_specs=pl.BlockSpec((block, 128), lambda i: (i, 0)),
        out_shape=jax.ShapeDtypeStruct((n, 128), BF16),
        compiler_params=params_of("arbitrary"),
        name="codes",
    )(nbr_t, mask_t)


def count_kernel(fan, halves, unroll, codes_ref, out_ref):
    nodes = codes_ref.shape[0]
    lane = lax.broadcasted_iota(jnp.int32, (16, 256), 1).astype(F32).astype(BF16)
    one = jnp.ones((16, 256), BF16)
    zero = jnp.zeros((16, 256), BF16)

    def group(g):
        at = pl.multiple_of(g * 16, 16)
        block = codes_ref[pl.ds(at, 16), :]
        low = [jnp.where(lane == block[:, k:k + 1], one, zero) for k in range(fan)]
        low = jnp.concatenate(low + [zero] * (16 - fan), axis=0)
        for h in range(halves):
            want = lane if h == halves - 1 else lane - 256
            high = [jnp.where(want == block[:, 16 + k:17 + k], one, zero) for k in range(fan)]
            high = jnp.concatenate(high + [zero] * (16 - fan), axis=0)
            got = lax.dot_general(high, low, (((0,), (0,)), ((), ())), preferred_element_type=F32).astype(BF16)
            for p in range(16):
                out_ref[pl.ds(at, 16), (h * 16 + p) * 256:(h * 16 + p + 1) * 256] = got[p * 16:p * 16 + 16, :]

    def step(s, carry):
        for u in range(unroll):
            group(s * unroll + u)
        return carry

    lax.fori_loop(0, nodes // (16 * unroll), step, 0)


def count_matrix(code, fan, vocab, block=256, unroll=4):
    n = code.shape[0]
    return pl.pallas_call(
        functools.partial(count_kernel, fan, vocab // 4096, unroll),
        grid=(n // block,),
        in_specs=[pl.BlockSpec((block, 128), lambda i: (i, 0))],
        out_specs=pl.BlockSpec((block, vocab), lambda i: (i, 0)),
        out_shape=jax.ShapeDtypeStruct((n, vocab), BF16),
        compiler_params=params_of("arbitrary"),
        cost_estimate=pl.CostEstimate(flops=2 * n * vocab * 256, bytes_accessed=2 * n * vocab, transcendentals=0),
        name="count_matrix",
    )(code)


def norm_rows(z, gain, shift):
    act = jnp.maximum(z, 0.0)
    mean_act = jnp.mean(act, axis=-1, keepdims=True)
    centred = act - mean_act
    var_act = jnp.mean(centred * centred, axis=-1, keepdims=True)
    return centred * lax.rsqrt(var_act + LN_EPS) * gain + shift


def norm_back(z, gain, d_out, axis):
    act = jnp.maximum(z, 0.0)
    mean_act = jnp.mean(act, axis=axis, keepdims=True)
    centred = act - mean_act
    var_act = jnp.mean(centred * centred, axis=axis, keepdims=True)
    inv = lax.rsqrt(var_act + LN_EPS)
    hat = centred * inv
    d_hat = d_out * gain
    mean_d = jnp.mean(d_hat, axis=axis, keepdims=True)
    mean_dh = jnp.mean(d_hat * hat, axis=axis, keepdims=True)
    d_act = (d_hat - mean_d - hat * mean_dh) * inv
    return jnp.where(z > 0.0, d_act, 0.0), d_out * hat


def layer_one_kernel(self_ids, m_ref, codes_ref, x_ref, w_self_ref, w_nbr_ref, vec_ref,
                     hs_ref, a_ref, h_ref, zt_ref, wide_ref, got_ref):
    block = m_ref.shape[0]
    rows, feat = x_ref.shape
    pid = pl.program_id(0)
    tiles = feat // 128

    @pl.when(pid == 0)
    def _():
        def spread(s, carry):
            at = pl.multiple_of(s * 128, 128)
            for c in range(tiles):
                wide_ref[pl.ds(at * 8 + c, 128, stride=8), :] = x_ref[pl.ds(at, 128), c * 128:(c + 1) * 128].astype(F32)
            return carry
        lax.fori_loop(0, rows // 128, spread, 0)

    def fetch(s, carry):
        for u in range(32):
            at = s * 32 + u
            idx = self_ids[pid * block + at]
            got_ref[pl.ds(pl.multiple_of(at * 8, 8), 8), :] = wide_ref[pl.ds(pl.multiple_of(idx * 8, 8), 8), :]
        return carry
    lax.fori_loop(0, block // 32, fetch, 0)
    for c in range(tiles):
        hs_ref[:, c * 128:(c + 1) * 128] = got_ref[pl.ds(c, block, stride=8), :].astype(BF16)
    count = codes_ref[:, 32:33].astype(F32)
    for c in range(feat // 256):
        cols = slice(c * 256, (c + 1) * 256)
        acc = jnp.dot(m_ref[...], x_ref[:, cols], preferred_element_type=F32)
        a_ref[:, cols] = (acc / count).astype(BF16)
    z = (jnp.dot(hs_ref[...], w_self_ref[...], preferred_element_type=F32)
         + jnp.dot(a_ref[...], w_nbr_ref[...], preferred_element_type=F32) + vec_ref[0:1, :])
    h_ref[...] = norm_rows(z, vec_ref[1:2, :], vec_ref[2:3, :]).astype(BF16)
    zt_ref[...] = z.T


def layer_one(m_one, code, table, self_ids, w_self, w_nbr, vecs, block=512):
    n, rows = m_one.shape
    feat = table.shape[1]
    whole = lambda i, ids: (0, 0)
    by_row = lambda i, ids: (i, 0)
    return pl.pallas_call(
        layer_one_kernel,
        grid_spec=pltpu.PrefetchScalarGridSpec(
            num_scalar_prefetch=1,
            grid=(n // block,),
            in_specs=[pl.BlockSpec((block, rows), by_row),
                      pl.BlockSpec((block, 128), by_row),
                      pl.BlockSpec((rows, feat), whole),
                      pl.BlockSpec((feat, HIDDEN), whole),
                      pl.BlockSpec((feat, HIDDEN), whole),
                      pl.BlockSpec((8, HIDDEN), whole)],
            out_specs=[pl.BlockSpec((block, feat), by_row),
                       pl.BlockSpec((block, feat), by_row),
                       pl.BlockSpec((block, HIDDEN), by_row),
                       pl.BlockSpec((HIDDEN, block), lambda i, ids: (0, i))],
            scratch_shapes=[pltpu.VMEM((rows * 8, 128), F32), pltpu.VMEM((block * 8, 128), F32)]),
        out_shape=[jax.ShapeDtypeStruct((n, feat), BF16),
                   jax.ShapeDtypeStruct((n, feat), BF16),
                   jax.ShapeDtypeStruct((n, HIDDEN), BF16),
                   jax.ShapeDtypeStruct((HIDDEN, n), F32)],
        compiler_params=params_of("arbitrary"),
        cost_estimate=pl.CostEstimate(flops=2 * n * rows * feat, bytes_accessed=2 * n * rows, transcendentals=0),
        name="layer_one",
    )(self_ids, m_one, code, table, w_self, w_nbr, vecs)


def layer_two_kernel(m_ref, codes_ref, h_all_ref, h_self_ref, w_self_ref, w_nbr_ref, vec_ref, a_ref, h_ref, z_ref):
    count = codes_ref[:, 32:33].astype(F32)
    acc = jnp.dot(m_ref[...], h_all_ref[...], preferred_element_type=F32)
    a_ref[...] = (acc / count).astype(BF16)
    z = (jnp.dot(h_self_ref[...], w_self_ref[...], preferred_element_type=F32)
         + jnp.dot(a_ref[...], w_nbr_ref[...], preferred_element_type=F32) + vec_ref[0:1, :])
    z_ref[...] = z
    h_ref[...] = norm_rows(z, vec_ref[1:2, :], vec_ref[2:3, :]).astype(BF16)


def layer_two(m_two, code, h_one, w_self, w_nbr, vecs, block=512):
    n, rows = m_two.shape
    whole = lambda i: (0, 0)
    by_row = lambda i: (i, 0)
    return pl.pallas_call(
        layer_two_kernel,
        grid=(n // block,),
        in_specs=[pl.BlockSpec((block, rows), by_row),
                  pl.BlockSpec((block, 128), by_row),
                  pl.BlockSpec((rows, HIDDEN), whole),
                  pl.BlockSpec((block, HIDDEN), by_row),
                  pl.BlockSpec((HIDDEN, HIDDEN), whole),
                  pl.BlockSpec((HIDDEN, HIDDEN), whole),
                  pl.BlockSpec((8, HIDDEN), whole)],
        out_specs=[pl.BlockSpec((block, HIDDEN), by_row)] * 3,
        out_shape=[jax.ShapeDtypeStruct((n, HIDDEN), BF16),
                   jax.ShapeDtypeStruct((n, HIDDEN), BF16),
                   jax.ShapeDtypeStruct((n, HIDDEN), F32)],
        compiler_params=params_of("arbitrary"),
        cost_estimate=pl.CostEstimate(flops=2 * n * rows * HIDDEN, bytes_accessed=2 * n * rows, transcendentals=0),
        name="layer_two",
    )(m_two, code, h_one, h_one, w_self, w_nbr, vecs)


def tdot(lhs, rhs):
    return lax.dot_general(lhs, rhs, (((0,), (0,)), ((), ())), preferred_element_type=F32)


def dot_t(lhs, rhs):
    return lax.dot_general(lhs, rhs, (((1,), (1,)), ((), ())), preferred_element_type=F32)


def top_kernel(classes, nbr3_ref, mask3_ref, label_ref, valid_ref, h2_ref, a2_ref, z2_ref, h1_ref, codes2_ref,
               w3s_ref, w3n_ref, w2s_ref, w2n_ref, vec_ref,
               g3s_ref, g3n_ref, g2s_ref, g2n_ref, vout_ref, dself_ref, dagg_ref, m3_ref, dh2_ref):
    seeds = nbr3_ref.shape[0]
    n_two = h2_ref.shape[0]
    fan = nbr3_ref.shape[1]
    piece = 512
    count3 = jnp.maximum(jnp.sum(mask3_ref[...], axis=1, keepdims=True), 1).astype(F32)
    for c in range(n_two // piece):
        ids = lax.broadcasted_iota(jnp.int32, (seeds, piece), 1) + c * piece
        acc = jnp.zeros((seeds, piece), F32)
        for k in range(fan):
            want = jnp.where(mask3_ref[:, k:k + 1] > 0, nbr3_ref[:, k:k + 1], -1)
            acc = acc + jnp.where(ids == want, 1.0, 0.0)
        m3_ref[:, c * piece:(c + 1) * piece] = acc.astype(BF16)
    a3 = (jnp.dot(m3_ref[...], h2_ref[...], preferred_element_type=F32) / count3).astype(BF16)
    self3 = h2_ref[0:seeds, :]
    logits = (jnp.dot(self3, w3s_ref[...], preferred_element_type=F32)
              + jnp.dot(a3, w3n_ref[...], preferred_element_type=F32) + vec_ref[3:4, :])
    col = lax.broadcasted_iota(jnp.int32, logits.shape, 1)
    real = col < classes
    top = jnp.max(jnp.where(real, logits, -jnp.inf), axis=1, keepdims=True)
    powers = jnp.where(real, jnp.exp(logits - top), 0.0)
    total = jnp.sum(powers, axis=1, keepdims=True)
    log_norm = top + jnp.log(total)
    hot = col == label_ref[...]
    picked = jnp.sum(jnp.where(hot, logits, 0.0), axis=1, keepdims=True)
    valid = valid_ref[...].astype(F32)
    loss = jnp.sum((log_norm - picked) * valid, axis=0, keepdims=True)
    n_valid = jnp.sum(valid, axis=0, keepdims=True)
    d_logits = (jnp.where(real, jnp.exp(logits - log_norm), 0.0) - jnp.where(hot, 1.0, 0.0)) * valid
    d_logb = d_logits.astype(BF16)
    g3s_ref[...] = tdot(self3, d_logb)
    g3n_ref[...] = tdot(a3, d_logb)
    d_self3 = dot_t(d_logb, w3s_ref[...])
    d_agg3 = (dot_t(d_logb, w3n_ref[...]) / count3).astype(BF16)
    dh2_ref[...] = tdot(m3_ref[...], d_agg3)
    dh2_ref[0:seeds, :] += d_self3
    d_h2 = dh2_ref[...]
    d_z2, gain_terms = norm_back(z2_ref[...], vec_ref[1:2, :], d_h2, -1)
    vout_ref[0:1, :] = jnp.sum(d_z2, axis=0, keepdims=True)
    vout_ref[1:2, :] = jnp.sum(gain_terms, axis=0, keepdims=True)
    vout_ref[2:3, :] = jnp.sum(d_h2, axis=0, keepdims=True)
    vout_ref[3:4, :] = jnp.sum(d_logits, axis=0, keepdims=True)
    vout_ref[4:5, :] = jnp.broadcast_to(loss, (1, HIDDEN))
    vout_ref[5:6, :] = jnp.broadcast_to(n_valid, (1, HIDDEN))
    vout_ref[6:8, :] = jnp.zeros((2, HIDDEN), F32)
    d_z2b = d_z2.astype(BF16)
    g2s_ref[...] = tdot(h1_ref[...], d_z2b)
    g2n_ref[...] = tdot(a2_ref[...], d_z2b)
    dself_ref[...] = dot_t(d_z2b, w2s_ref[...]).T
    count2 = codes2_ref[:, 32:33].astype(F32)
    dagg_ref[...] = (dot_t(d_z2b, w2n_ref[...]) / count2).T.astype(BF16)


def top(classes, nbr3, mask3, label, valid, h2, a2, z2, h1, codes2, w3s, w3n, w2s, w2n, vecs):
    n_two = h2.shape[0]
    seeds = nbr3.shape[0]
    square = jax.ShapeDtypeStruct((HIDDEN, HIDDEN), F32)
    full = lambda x: pl.BlockSpec(x.shape, lambda i: (0, 0))
    args = (nbr3, mask3, label, valid, h2, a2, z2, h1, codes2, w3s, w3n, w2s, w2n, vecs)
    outs = [square, square, square, square, jax.ShapeDtypeStruct((8, HIDDEN), F32),
            jax.ShapeDtypeStruct((HIDDEN, n_two), F32), jax.ShapeDtypeStruct((HIDDEN, n_two), BF16)]
    specs = [full(x) for x in args]
    specs[7] = pl.BlockSpec((n_two, HIDDEN), lambda i: (0, 0))
    return pl.pallas_call(
        functools.partial(top_kernel, classes),
        grid=(1,),
        in_specs=specs,
        out_specs=[full(x) for x in outs],
        out_shape=outs,
        scratch_shapes=[pltpu.VMEM((seeds, n_two), BF16), pltpu.VMEM((n_two, HIDDEN), F32)],
        compiler_params=params_of("arbitrary"),
        name="layer_three",
    )(*args)


def bottom_kernel(dagg_ref, m_ref, dself_ref, zt_ref, hs_ref, a_ref, gain_ref,
                  gs_ref, gn_ref, vout_ref):
    pid = pl.program_id(0)
    block = m_ref.shape[1]
    n_self = dself_ref.shape[1] // block

    @pl.when(pid == 0)
    def _():
        gs_ref[...] = jnp.zeros_like(gs_ref)
        gn_ref[...] = jnp.zeros_like(gn_ref)
        vout_ref[...] = jnp.zeros_like(vout_ref)

    d_h = jnp.dot(dagg_ref[...], m_ref[...], preferred_element_type=F32)
    at = pl.multiple_of(jnp.minimum(pid, n_self - 1) * block, block)
    d_h = d_h + jnp.where(pid < n_self, dself_ref[:, pl.ds(at, block)], 0.0)
    d_z, gain_terms = norm_back(zt_ref[...], gain_ref[:, 0:1], d_h, 0)
    sums = [jnp.sum(term, axis=1, keepdims=True) for term in (d_z, gain_terms, d_h)]
    lane = lax.broadcasted_iota(jnp.int32, (HIDDEN, 128), 1)
    vout_ref[...] += jnp.where(lane == 0, sums[0], jnp.where(lane == 1, sums[1], jnp.where(lane == 2, sums[2], 0.0)))
    d_zb = d_z.astype(BF16)
    gs_ref[...] += jnp.dot(d_zb, hs_ref[...], preferred_element_type=F32)
    gn_ref[...] += jnp.dot(d_zb, a_ref[...], preferred_element_type=F32)


def bottom(dagg_t, m_two, dself_t, z_t, h_self, a_one, gain_col, block=512):
    n_two, n = m_two.shape
    feat = h_self.shape[1]
    whole = lambda i: (0, 0)
    grads = jax.ShapeDtypeStruct((HIDDEN, feat), F32)
    return pl.pallas_call(
        bottom_kernel,
        grid=(n // block,),
        in_specs=[pl.BlockSpec((HIDDEN, n_two), whole),
                  pl.BlockSpec((n_two, block), lambda i: (0, i)),
                  pl.BlockSpec((HIDDEN, n_two), whole),
                  pl.BlockSpec((HIDDEN, block), lambda i: (0, i)),
                  pl.BlockSpec((block, feat), lambda i: (i, 0)),
                  pl.BlockSpec((block, feat), lambda i: (i, 0)),
                  pl.BlockSpec((HIDDEN, 128), whole)],
        out_specs=[pl.BlockSpec((HIDDEN, feat), whole), pl.BlockSpec((HIDDEN, feat), whole),
                   pl.BlockSpec((HIDDEN, 128), whole)],
        out_shape=[grads, grads, jax.ShapeDtypeStruct((HIDDEN, 128), F32)],
        compiler_params=params_of("arbitrary"),
        cost_estimate=pl.CostEstimate(flops=2 * n * n_two * HIDDEN, bytes_accessed=2 * n * n_two, transcendentals=0),
        name="layer_one_back",
    )(dagg_t, m_two, dself_t, z_t, h_self, a_one, gain_col)


def adam_update(params, adam_m, adam_v, grads):
    m_new = BETA_ONE * adam_m + (1.0 - BETA_ONE) * grads
    v_new = BETA_TWO * adam_v + (1.0 - BETA_TWO) * grads * grads
    m_hat = m_new / (1.0 - BETA_ONE ** STEP)
    v_hat = v_new / (1.0 - BETA_TWO ** STEP)
    return (params - ADAM_LR * m_hat / (jnp.sqrt(v_hat) + ADAM_EPS), m_new, v_new)


def stack_rows(*rows):
    width = HIDDEN
    rows = [jnp.pad(row, (0, width - row.shape[0])) for row in rows]
    rows += [jnp.zeros((width,), F32)] * (8 - len(rows))
    return jnp.stack(rows)


def solution(mesh):
    def body(feats, frontier, nbr_l1, mask_l1, nbr_l2, mask_l2, nbr_l3, mask_l3, labels, seed_mask, params, adam_m, adam_v):
        feat = feats.shape[1]
        classes = class_count(params.shape[0], feat)
        n_one = nbr_l1.shape[0]
        table = lax.all_gather(feats, 'dp', axis=0, tiled=True)
        pieces = unpack(params, feat, classes)
        pad3 = ((0, 0), (0, HIDDEN - classes))
        w3s = jnp.pad(pieces[10], pad3).astype(BF16)
        w3n = jnp.pad(pieces[11], pad3).astype(BF16)
        code_one = compose(frontier, nbr_l1.T, mask_l1.T)
        code_two = codes(nbr_l2.T, mask_l2.T, 256)
        m_one = count_matrix(code_one, nbr_l1.shape[1], table.shape[0])
        m_two = count_matrix(code_two, nbr_l2.shape[1], n_one)
        h_self, a_one, h_one, z_one_t = layer_one(
            m_one, code_one, table, frontier[:n_one], pieces[0].astype(BF16), pieces[1].astype(BF16),
            stack_rows(pieces[2], pieces[3], pieces[4]))
        a_two, h_two, z_two = layer_two(m_two, code_two, h_one, pieces[5].astype(BF16), pieces[6].astype(BF16),
                                        stack_rows(pieces[7], pieces[8], pieces[9]))
        g3s, g3n, g2s, g2n, vout, dself_t, dagg_t = top(
            classes, nbr_l3, mask_l3, labels[:, None], seed_mask[:, None], h_two, a_two, z_two, h_one, code_two,
            w3s, w3n, pieces[5].astype(BF16), pieces[6].astype(BF16),
            stack_rows(pieces[7], pieces[8], pieces[9], pieces[12]))
        gain_col = jnp.broadcast_to(pieces[3][:, None], (HIDDEN, 128))
        g1s, g1n, vone = bottom(dagg_t, m_two, dself_t, z_one_t, h_self, a_one, gain_col)
        sums = jnp.concatenate([
            g1s.T.reshape(-1), g1n.T.reshape(-1), vone[:, 0], vone[:, 1], vone[:, 2],
            g2s.reshape(-1), g2n.reshape(-1), vout[0], vout[1], vout[2],
            g3s[:, :classes].reshape(-1), g3n[:, :classes].reshape(-1), vout[3, :classes],
            vout[4, :1], vout[5, :1]])
        sums = lax.psum(sums, 'dp')
        total = jnp.maximum(sums[-1], 1.0)
        loss = sums[-2] / total
        return (loss,) + adam_update(params, adam_m, adam_v, sums[:-2] / total)

    row_spec = P('dp')
    replicated = P()
    return jax.shard_map(body, mesh=mesh, in_specs=(row_spec,) * 10 + (replicated,) * 3,
                         out_specs=(replicated,) * 4, check_vma=False)
```

```python
import functools

import jax
import jax.numpy as jnp
from jax import lax
from jax.experimental import pallas as pl
from jax.experimental.pallas import tpu as pltpu
from jax.sharding import PartitionSpec as P

HIDDEN = 256
STEP = 10
LN_EPS = 1e-5
BETA_ONE = 0.9
BETA_TWO = 0.999
ADAM_LR = 3e-3
ADAM_EPS = 1e-8
F32 = jnp.float32
BF16 = jnp.bfloat16
VMEM_ALL = 60 * 1024 * 1024


def param_shapes(feat, classes):
    return [(feat, HIDDEN), (feat, HIDDEN), (HIDDEN,), (HIDDEN,), (HIDDEN,),
            (HIDDEN, HIDDEN), (HIDDEN, HIDDEN), (HIDDEN,), (HIDDEN,), (HIDDEN,),
            (HIDDEN, classes), (HIDDEN, classes), (classes,)]


def class_count(n_params, feat):
    return (n_params - 2 * feat * HIDDEN - 6 * HIDDEN - 2 * HIDDEN * HIDDEN) // (2 * HIDDEN + 1)


def unpack(flat, feat, classes):
    pieces = []
    offset = 0
    for pshape in param_shapes(feat, classes):
        count_el = 1
        for extent in pshape:
            count_el = count_el * extent
        pieces.append(flat[offset:offset + count_el].reshape(pshape))
        offset = offset + count_el
    return pieces


def params_of(*sem, vmem=VMEM_ALL):
    return pltpu.CompilerParams(dimension_semantics=sem, vmem_limit_bytes=vmem)


def emit_codes(lo, hi, mask, shift, low_ref, high_ref, count_ref):
    n = lo.shape[1]
    node = (lax.broadcasted_iota(jnp.int32, (16, n), 1) & 15).astype(F32)
    code = jnp.where(mask > 0, hi * 16.0 + node - shift, -384.0)
    count = jnp.maximum(jnp.sum(mask, axis=0, keepdims=True), 1).astype(F32)
    mine = (lax.broadcasted_iota(jnp.int32, (8, 128), 1) >> 4) == lax.broadcasted_iota(jnp.int32, (8, 128), 0)
    fold = ((lax.broadcasted_iota(jnp.int32, (128, 256), 0) & 15)
            == (lax.broadcasted_iota(jnp.int32, (128, 256), 1) & 15)).astype(F32).astype(BF16)
    part = lax.broadcasted_iota(jnp.int32, (8, 256), 1) >> 4
    for c in range(n // 128):
        lanes = slice(c * 128, (c + 1) * 128)
        count_ref[lanes, :] = jnp.broadcast_to(count[:, lanes], (128, 128)).T
        for value, ref in ((lo, low_ref), (code, high_ref)):
            spread = jnp.concatenate([jnp.where(mine, jnp.broadcast_to(value[k:k + 1, lanes], (8, 128)), 0.0)
                                      for k in range(16)], axis=0)
            folded = jnp.dot(spread.astype(BF16), fold, preferred_element_type=F32)
            rows = folded[0:8, :]
            for k in range(1, 16):
                rows = jnp.where(part == k, folded[k * 8:k * 8 + 8, :], rows)
            ref[c * 8:c * 8 + 8, :] = rows


def pad_rows(x, rows):
    return jnp.concatenate([x, jnp.zeros((rows - x.shape[0], x.shape[1]), x.dtype)], axis=0)


def compose_kernel(front_ref, nbr_ref, mask_ref, low_ref, high_ref, count_ref, table_ref):
    fan, n = nbr_ref.shape

    @pl.when(pl.program_id(0) == 0)
    def _():
        ids = front_ref[...]
        table_ref[0:128, :] = (ids & 255).astype(F32).T.astype(BF16)
        table_ref[128:256, :] = (ids >> 8).astype(F32).T.astype(BF16)

    row = lax.broadcasted_iota(jnp.int32, (256, n), 0).astype(F32).astype(BF16)
    one = jnp.ones((16, n), BF16)
    zero = jnp.zeros((16, n), BF16)
    sub = lax.broadcasted_iota(jnp.int32, (8, n), 0)
    lows, highs = [], []
    for k in range(fan):
        nbr = nbr_ref[k:k + 1, :]
        want = jnp.broadcast_to((nbr >> 7).astype(F32), (16, n)).astype(BF16)
        pick = jnp.concatenate([jnp.where(row[p * 16:p * 16 + 16, :] == want, one, zero) for p in range(16)], axis=0)
        cand = jnp.dot(table_ref[...], pick, preferred_element_type=F32)
        lane = jnp.broadcast_to(nbr & 127, (8, n))
        low = jnp.zeros((8, n), F32)
        high = jnp.zeros((8, n), F32)
        for p in range(16):
            hit = sub + p * 8 == lane
            low = jnp.where(hit, cand[p * 8:p * 8 + 8, :], low)
            high = jnp.where(hit, cand[128 + p * 8:136 + p * 8, :], high)
        lows.append(jnp.sum(low, axis=0, keepdims=True))
        highs.append(jnp.sum(high, axis=0, keepdims=True))
    fill = [jnp.zeros((1, n), F32)] * (16 - fan)
    emit_codes(jnp.concatenate(lows + fill, axis=0), jnp.concatenate(highs + fill, axis=0),
               pad_rows(mask_ref[...], 16), 0.0, low_ref, high_ref, count_ref)


def codes_kernel(shift, nbr_ref, mask_ref, low_ref, high_ref, count_ref):
    ids = pad_rows(nbr_ref[...], 16)
    emit_codes((ids & 255).astype(F32), (ids >> 8).astype(F32), pad_rows(mask_ref[...], 16), shift,
               low_ref, high_ref, count_ref)


def code_outs(n, block):
    rows = pl.BlockSpec((block // 16, 256), lambda i: (i, 0))
    shape = jax.ShapeDtypeStruct((n // 16, 256), F32)
    return dict(out_specs=[rows, rows, pl.BlockSpec((block, 128), lambda i: (i, 0))],
                out_shape=[shape, shape, jax.ShapeDtypeStruct((n, 128), F32)])


def compose(frontier, nbr_t, mask_t, block=512):
    fan, n = nbr_t.shape
    rows = frontier.shape[0] // 128
    return pl.pallas_call(
        compose_kernel,
        grid=(n // block,),
        in_specs=[pl.BlockSpec((rows, 128), lambda i: (0, 0)),
                  pl.BlockSpec((fan, block), lambda i: (0, i)),
                  pl.BlockSpec((fan, block), lambda i: (0, i))],
        **code_outs(n, block),
        scratch_shapes=[pltpu.VMEM((256, rows), BF16)],
        compiler_params=params_of("arbitrary"),
        cost_estimate=pl.CostEstimate(flops=2 * 65536 * fan * n, bytes_accessed=10**7, transcendentals=0),
        name="compose_ids",
    )(frontier.reshape(rows, 128), nbr_t, mask_t)


def codes(nbr_t, mask_t, shift, block=512):
    fan, n = nbr_t.shape
    return pl.pallas_call(
        functools.partial(codes_kernel, shift),
        grid=(n // block,),
        in_specs=[pl.BlockSpec((fan, block), lambda i: (0, i)),
                  pl.BlockSpec((fan, block), lambda i: (0, i))],
        **code_outs(n, block),
        compiler_params=params_of("arbitrary"),
        name="codes",
    )(nbr_t, mask_t)


def count_kernel(halves, unroll, low_ref, high_ref, out_ref):
    nodes = out_ref.shape[0]
    row = lax.broadcasted_iota(jnp.int32, (256, 256), 0).astype(F32).astype(BF16)
    one = jnp.ones((16, 256), BF16)
    zero = jnp.zeros((16, 256), BF16)

    def one_hot(want, less):
        return [jnp.where(row[p * 16:p * 16 + 16, :] - less == want, one, zero) for p in range(16)]

    def group(g):
        at = pl.multiple_of(g * 16, 16)
        low = jnp.concatenate(one_hot(jnp.broadcast_to(low_ref[pl.ds(g, 1), :], (16, 256)).astype(BF16), 0), axis=0)
        want = jnp.broadcast_to(high_ref[pl.ds(g, 1), :], (16, 256)).astype(BF16)
        high = []
        for h in range(halves):
            high += one_hot(want, 0 if h == halves - 1 else 256)
        got = dot_t(jnp.concatenate(high, axis=0), low).astype(BF16)
        for p in range(16 * halves):
            out_ref[pl.ds(at, 16), p * 256:(p + 1) * 256] = got[p * 16:p * 16 + 16, :]

    def step(s, carry):
        for u in range(unroll):
            group(s * unroll + u)
        return carry

    lax.fori_loop(0, nodes // (16 * unroll), step, 0)


def count_matrix(code, vocab, block=256, unroll=16):
    low, high, _ = code
    n = low.shape[0] * 16
    rows = pl.BlockSpec((block // 16, 256), lambda i: (i, 0))
    return pl.pallas_call(
        functools.partial(count_kernel, vocab // 4096, unroll),
        grid=(n // block,),
        in_specs=[rows, rows],
        out_specs=pl.BlockSpec((block, vocab), lambda i: (i, 0)),
        out_shape=jax.ShapeDtypeStruct((n, vocab), BF16),
        compiler_params=params_of("arbitrary"),
        cost_estimate=pl.CostEstimate(flops=2 * n * vocab * 256, bytes_accessed=2 * n * vocab, transcendentals=0),
        name="count_matrix",
    )(low, high)


def norm_rows(z, gain, shift):
    act = jnp.maximum(z, 0.0)
    mean_act = jnp.mean(act, axis=-1, keepdims=True)
    centred = act - mean_act
    var_act = jnp.mean(centred * centred, axis=-1, keepdims=True)
    return centred * lax.rsqrt(var_act + LN_EPS) * gain + shift


def norm_back(z, gain, d_out, axis):
    act = jnp.maximum(z, 0.0)
    mean_act = jnp.mean(act, axis=axis, keepdims=True)
    centred = act - mean_act
    var_act = jnp.mean(centred * centred, axis=axis, keepdims=True)
    inv = lax.rsqrt(var_act + LN_EPS)
    hat = centred * inv
    d_hat = d_out * gain
    mean_d = jnp.mean(d_hat, axis=axis, keepdims=True)
    mean_dh = jnp.mean(d_hat * hat, axis=axis, keepdims=True)
    d_act = (d_hat - mean_d - hat * mean_dh) * inv
    return jnp.where(z > 0.0, d_act, 0.0), d_out * hat


def layer_one_kernel(self_ids, m_ref, codes_ref, x_ref, w_self_ref, w_nbr_ref, vec_ref,
                     hs_ref, a_ref, h_ref, zt_ref, wide_ref, got_ref):
    block = m_ref.shape[0]
    rows, feat = x_ref.shape
    pid = pl.program_id(0)
    tiles = feat // 128

    @pl.when(pid == 0)
    def _():
        def spread(s, carry):
            at = pl.multiple_of(s * 128, 128)
            for c in range(tiles):
                wide_ref[pl.ds(at * 8 + c, 128, stride=8), :] = x_ref[pl.ds(at, 128), c * 128:(c + 1) * 128].astype(F32)
            return carry
        lax.fori_loop(0, rows // 128, spread, 0)

    def fetch(s, carry):
        for u in range(32):
            at = s * 32 + u
            idx = self_ids[pid * block + at]
            got_ref[pl.ds(pl.multiple_of(at * 8, 8), 8), :] = wide_ref[pl.ds(pl.multiple_of(idx * 8, 8), 8), :]
        return carry
    lax.fori_loop(0, block // 32, fetch, 0)
    for c in range(tiles):
        hs_ref[:, c * 128:(c + 1) * 128] = got_ref[pl.ds(c, block, stride=8), :].astype(BF16)
    count = codes_ref[:, 0:1]
    for c in range(feat // 256):
        cols = slice(c * 256, (c + 1) * 256)
        acc = jnp.dot(m_ref[...], x_ref[:, cols], preferred_element_type=F32)
        a_ref[:, cols] = (acc / count).astype(BF16)
    z = (jnp.dot(hs_ref[...], w_self_ref[...], preferred_element_type=F32)
         + jnp.dot(a_ref[...], w_nbr_ref[...], preferred_element_type=F32) + vec_ref[0:1, :])
    h_ref[...] = norm_rows(z, vec_ref[1:2, :], vec_ref[2:3, :]).astype(BF16)
    zt_ref[...] = z.T


def layer_one(m_one, code, table, self_ids, w_self, w_nbr, vecs, block=512):
    n, rows = m_one.shape
    feat = table.shape[1]
    whole = lambda i, ids: (0, 0)
    by_row = lambda i, ids: (i, 0)
    return pl.pallas_call(
        layer_one_kernel,
        grid_spec=pltpu.PrefetchScalarGridSpec(
            num_scalar_prefetch=1,
            grid=(n // block,),
            in_specs=[pl.BlockSpec((block, rows), by_row),
                      pl.BlockSpec((block, 128), by_row),
                      pl.BlockSpec((rows, feat), whole),
                      pl.BlockSpec((feat, HIDDEN), whole),
                      pl.BlockSpec((feat, HIDDEN), whole),
                      pl.BlockSpec((8, HIDDEN), whole)],
            out_specs=[pl.BlockSpec((block, feat), by_row),
                       pl.BlockSpec((block, feat), by_row),
                       pl.BlockSpec((block, HIDDEN), by_row),
                       pl.BlockSpec((HIDDEN, block), lambda i, ids: (0, i))],
            scratch_shapes=[pltpu.VMEM((rows * 8, 128), F32), pltpu.VMEM((block * 8, 128), F32)]),
        out_shape=[jax.ShapeDtypeStruct((n, feat), BF16),
                   jax.ShapeDtypeStruct((n, feat), BF16),
                   jax.ShapeDtypeStruct((n, HIDDEN), BF16),
                   jax.ShapeDtypeStruct((HIDDEN, n), F32)],
        compiler_params=params_of("arbitrary"),
        cost_estimate=pl.CostEstimate(flops=2 * n * rows * feat, bytes_accessed=2 * n * rows, transcendentals=0),
        name="layer_one",
    )(self_ids, m_one, code, table, w_self, w_nbr, vecs)


def layer_two_kernel(m_ref, codes_ref, h_all_ref, h_self_ref, w_self_ref, w_nbr_ref, vec_ref, a_ref, h_ref, z_ref):
    count = codes_ref[:, 0:1]
    acc = jnp.dot(m_ref[...], h_all_ref[...], preferred_element_type=F32)
    a_ref[...] = (acc / count).astype(BF16)
    z = (jnp.dot(h_self_ref[...], w_self_ref[...], preferred_element_type=F32)
         + jnp.dot(a_ref[...], w_nbr_ref[...], preferred_element_type=F32) + vec_ref[0:1, :])
    z_ref[...] = z
    h_ref[...] = norm_rows(z, vec_ref[1:2, :], vec_ref[2:3, :]).astype(BF16)


def layer_two(m_two, code, h_one, w_self, w_nbr, vecs, block=512):
    n, rows = m_two.shape
    whole = lambda i: (0, 0)
    by_row = lambda i: (i, 0)
    return pl.pallas_call(
        layer_two_kernel,
        grid=(n // block,),
        in_specs=[pl.BlockSpec((block, rows), by_row),
                  pl.BlockSpec((block, 128), by_row),
                  pl.BlockSpec((rows, HIDDEN), whole),
                  pl.BlockSpec((block, HIDDEN), by_row),
                  pl.BlockSpec((HIDDEN, HIDDEN), whole),
                  pl.BlockSpec((HIDDEN, HIDDEN), whole),
                  pl.BlockSpec((8, HIDDEN), whole)],
        out_specs=[pl.BlockSpec((block, HIDDEN), by_row)] * 3,
        out_shape=[jax.ShapeDtypeStruct((n, HIDDEN), BF16),
                   jax.ShapeDtypeStruct((n, HIDDEN), BF16),
                   jax.ShapeDtypeStruct((n, HIDDEN), F32)],
        compiler_params=params_of("arbitrary"),
        cost_estimate=pl.CostEstimate(flops=2 * n * rows * HIDDEN, bytes_accessed=2 * n * rows, transcendentals=0),
        name="layer_two",
    )(m_two, code, h_one, h_one, w_self, w_nbr, vecs)


def tdot(lhs, rhs):
    return lax.dot_general(lhs, rhs, (((0,), (0,)), ((), ())), preferred_element_type=F32)


def dot_t(lhs, rhs):
    return lax.dot_general(lhs, rhs, (((1,), (1,)), ((), ())), preferred_element_type=F32)


def put_rows(ref, at, mat):
    n = mat.shape[0]
    ref[pl.ds(at, n, stride=2), :] = mat[:, 0:128]
    ref[pl.ds(at + 1, n, stride=2), :] = mat[:, 128:256]


def put_vector(ref, at, row):
    ref[at:at + 1, :] = row[:, 0:128]
    ref[at + 1:at + 2, :] = row[:, 128:256]


def top_kernel(classes, nbr3_ref, mask3_ref, label_ref, valid_ref, h2_ref, a2_ref, z2_ref, h1_ref, codes2_ref,
               w3s_ref, w3n_ref, w2s_ref, w2n_ref, vec_ref,
               g3s_ref, g3n_ref, rows_ref, vout_ref, dself_ref, dagg_ref, m3_ref, dh2_ref):
    seeds = nbr3_ref.shape[0]
    n_two = h2_ref.shape[0]
    fan = nbr3_ref.shape[1]
    piece = 512
    count3 = jnp.maximum(jnp.sum(mask3_ref[...], axis=1, keepdims=True), 1).astype(F32)
    for c in range(n_two // piece):
        ids = lax.broadcasted_iota(jnp.int32, (seeds, piece), 1) + c * piece
        acc = jnp.zeros((seeds, piece), F32)
        for k in range(fan):
            want = jnp.where(mask3_ref[:, k:k + 1] > 0, nbr3_ref[:, k:k + 1], -1)
            acc = acc + jnp.where(ids == want, 1.0, 0.0)
        m3_ref[:, c * piece:(c + 1) * piece] = acc.astype(BF16)
    a3 = (jnp.dot(m3_ref[...], h2_ref[...], preferred_element_type=F32) / count3).astype(BF16)
    self3 = h2_ref[0:seeds, :]
    logits = (jnp.dot(self3, w3s_ref[...], preferred_element_type=F32)
              + jnp.dot(a3, w3n_ref[...], preferred_element_type=F32) + vec_ref[3:4, :])
    col = lax.broadcasted_iota(jnp.int32, logits.shape, 1)
    real = col < classes
    top = jnp.max(jnp.where(real, logits, -jnp.inf), axis=1, keepdims=True)
    powers = jnp.where(real, jnp.exp(logits - top), 0.0)
    total = jnp.sum(powers, axis=1, keepdims=True)
    log_norm = top + jnp.log(total)
    hot = col == label_ref[...]
    picked = jnp.sum(jnp.where(hot, logits, 0.0), axis=1, keepdims=True)
    valid = valid_ref[...].astype(F32)
    loss = jnp.sum((log_norm - picked) * valid, axis=0, keepdims=True)
    n_valid = jnp.sum(valid, axis=0, keepdims=True)
    d_logits = (jnp.where(real, jnp.exp(logits - log_norm), 0.0) - jnp.where(hot, 1.0, 0.0)) * valid
    d_logb = d_logits.astype(BF16)
    g3s_ref[...] = tdot(self3, d_logb)
    g3n_ref[...] = tdot(a3, d_logb)
    d_self3 = dot_t(d_logb, w3s_ref[...])
    d_agg3 = (dot_t(d_logb, w3n_ref[...]) / count3).astype(BF16)
    dh2_ref[...] = tdot(m3_ref[...], d_agg3)
    dh2_ref[0:seeds, :] += d_self3
    d_h2 = dh2_ref[...]
    d_z2, gain_terms = norm_back(z2_ref[...], vec_ref[1:2, :], d_h2, -1)
    vout_ref[0:1, :] = jnp.sum(d_logits, axis=0, keepdims=True)
    vout_ref[1:2, :] = jnp.broadcast_to(loss, (1, HIDDEN))
    vout_ref[2:3, :] = jnp.broadcast_to(n_valid, (1, HIDDEN))
    vout_ref[3:8, :] = jnp.zeros((5, HIDDEN), F32)
    d_z2b = d_z2.astype(BF16)
    put_rows(rows_ref, 0, tdot(h1_ref[...], d_z2b))
    put_rows(rows_ref, 2 * HIDDEN, tdot(a2_ref[...], d_z2b))
    for index, term in enumerate((d_z2, gain_terms, d_h2)):
        put_vector(rows_ref, 4 * HIDDEN + 2 * index, jnp.sum(term, axis=0, keepdims=True))
    rows_ref[4 * HIDDEN + 6:4 * HIDDEN + 8, :] = jnp.zeros((2, 128), F32)
    dself_ref[...] = dot_t(d_z2b, w2s_ref[...]).T
    count2 = codes2_ref[:, 0:1]
    dagg_ref[...] = (dot_t(d_z2b, w2n_ref[...]) / count2).T.astype(BF16)


def top(classes, nbr3, mask3, label, valid, h2, a2, z2, h1, codes2, w3s, w3n, w2s, w2n, vecs):
    n_two = h2.shape[0]
    seeds = nbr3.shape[0]
    square = jax.ShapeDtypeStruct((HIDDEN, HIDDEN), F32)
    rows = jax.ShapeDtypeStruct((4 * HIDDEN + 8, 128), F32)
    full = lambda x: pl.BlockSpec(x.shape, lambda i: (0, 0))
    args = (nbr3, mask3, label, valid, h2, a2, z2, h1, codes2, w3s, w3n, w2s, w2n, vecs)
    outs = [square, square, rows, jax.ShapeDtypeStruct((8, HIDDEN), F32),
            jax.ShapeDtypeStruct((HIDDEN, n_two), F32), jax.ShapeDtypeStruct((HIDDEN, n_two), BF16)]
    specs = [full(x) for x in args]
    specs[7] = pl.BlockSpec((n_two, HIDDEN), lambda i: (0, 0))
    return pl.pallas_call(
        functools.partial(top_kernel, classes),
        grid=(1,),
        in_specs=specs,
        out_specs=[full(x) for x in outs],
        out_shape=outs,
        scratch_shapes=[pltpu.VMEM((seeds, n_two), BF16), pltpu.VMEM((n_two, HIDDEN), F32)],
        compiler_params=params_of("arbitrary"),
        name="layer_three",
    )(*args)


def bottom_kernel(dagg_ref, m_ref, dself_ref, zt_ref, hs_ref, a_ref, gain_ref, rows_ref, gs_ref, gn_ref, vec_ref):
    pid = pl.program_id(0)
    block = m_ref.shape[1]
    feat = hs_ref.shape[1]
    n_self = dself_ref.shape[1] // block

    @pl.when(pid == 0)
    def _():
        gs_ref[...] = jnp.zeros_like(gs_ref)
        gn_ref[...] = jnp.zeros_like(gn_ref)
        vec_ref[...] = jnp.zeros_like(vec_ref)

    d_h = jnp.dot(dagg_ref[...], m_ref[...], preferred_element_type=F32)
    at = pl.multiple_of(jnp.minimum(pid, n_self - 1) * block, block)
    d_h = d_h + jnp.where(pid < n_self, dself_ref[:, pl.ds(at, block)], 0.0)
    d_z, gain_terms = norm_back(zt_ref[...], gain_ref[:, 0:1], d_h, 0)
    sums = [jnp.sum(term, axis=1, keepdims=True) for term in (d_z, gain_terms, d_h)]
    lane = lax.broadcasted_iota(jnp.int32, (HIDDEN, 128), 1)
    vec_ref[...] += jnp.where(lane == 0, sums[0], jnp.where(lane == 1, sums[1], jnp.where(lane == 2, sums[2], 0.0)))
    d_zb = d_z.astype(BF16)
    gs_ref[...] += jnp.dot(d_zb, hs_ref[...], preferred_element_type=F32)
    gn_ref[...] += jnp.dot(d_zb, a_ref[...], preferred_element_type=F32)

    @pl.when(pid == pl.num_programs(0) - 1)
    def _():
        put_rows(rows_ref, 0, gs_ref[...].T)
        put_rows(rows_ref, 2 * feat, gn_ref[...].T)
        vectors = vec_ref[...].T
        for index in range(3):
            put_vector(rows_ref, 4 * feat + 2 * index, vectors[index:index + 1, :])
        rows_ref[4 * feat + 6:4 * feat + 8, :] = jnp.zeros((2, 128), F32)


def bottom(dagg_t, m_two, dself_t, z_t, h_self, a_one, gain_col, block=512):
    n_two, n = m_two.shape
    feat = h_self.shape[1]
    whole = lambda i: (0, 0)
    rows = 4 * feat + 8
    return pl.pallas_call(
        bottom_kernel,
        grid=(n // block,),
        in_specs=[pl.BlockSpec((HIDDEN, n_two), whole),
                  pl.BlockSpec((n_two, block), lambda i: (0, i)),
                  pl.BlockSpec((HIDDEN, n_two), whole),
                  pl.BlockSpec((HIDDEN, block), lambda i: (0, i)),
                  pl.BlockSpec((block, feat), lambda i: (i, 0)),
                  pl.BlockSpec((block, feat), lambda i: (i, 0)),
                  pl.BlockSpec((HIDDEN, 128), whole)],
        out_specs=pl.BlockSpec((rows, 128), whole),
        out_shape=jax.ShapeDtypeStruct((rows, 128), F32),
        scratch_shapes=[pltpu.VMEM((HIDDEN, feat), F32), pltpu.VMEM((HIDDEN, feat), F32), pltpu.VMEM((HIDDEN, 128), F32)],
        compiler_params=params_of("arbitrary"),
        cost_estimate=pl.CostEstimate(flops=2 * n * n_two * HIDDEN, bytes_accessed=2 * n * n_two, transcendentals=0),
        name="layer_one_back",
    )(dagg_t, m_two, dself_t, z_t, h_self, a_one, gain_col)


CHUNKS = 4


def sum_kernel(low_ref, mid_ref, top_ref, out_ref, buf_ref, in0_ref, in1_ref, in2_ref, send_sem, recv_sem):
    me = lax.axis_index('dp')
    core = me % 2
    x_bit = (me // 2) % 2
    y_bit = me // 4
    x_peer = me + 2 - 4 * x_bit
    y_peer = me + 4 - 8 * y_bit
    mate = me + 1 - 2 * core
    first = x_bit + core * (y_bit - x_bit)
    second = y_bit + core * (x_bit - y_bit)
    peer_one = x_peer + core * (y_peer - x_peer)
    peer_two = y_peer + core * (x_peer - y_peer)
    barrier = pltpu.get_barrier_semaphore()
    for peer in (mate, x_peer, y_peer):
        pl.semaphore_signal(barrier, inc=1, device_id=(peer,), device_id_type=pl.DeviceIdType.MESH)
    n_low = low_ref.shape[0] - 2
    n_mid = mid_ref.shape[0] - 2
    n_top = top_ref.shape[0]
    buf_ref[0:n_low, :] = low_ref[0:n_low, :]
    buf_ref[n_low:n_low + n_mid, :] = mid_ref[0:n_mid, :]
    buf_ref[n_low + n_mid:n_low + n_mid + n_top, :] = top_ref[...]
    pl.semaphore_wait(barrier, 3)

    size = buf_ref.shape[0] // CHUNKS
    half, quarter, eighth = size // 2, size // 4, size // 8

    def rows(ref, at, count):
        return ref.at[pl.ds(pl.multiple_of(at, 8), count), :]

    def copy(chunk, phase):
        base = chunk * size + core * half
        if phase == 0:
            src, dst, peer = rows(buf_ref, chunk * size + (1 - core) * half, half), in0_ref.at[chunk], mate
        elif phase == 1:
            src, dst, peer = rows(buf_ref, base + (1 - first) * quarter, quarter), in1_ref.at[chunk], peer_one
        elif phase == 2:
            at = base + first * quarter + (1 - second) * eighth
            src, dst, peer = rows(buf_ref, at, eighth), in2_ref.at[chunk], peer_two
        elif phase == 3:
            at = base + first * quarter + second * eighth
            src, dst, peer = rows(out_ref, at, eighth), rows(out_ref, at, eighth), peer_two
        elif phase == 4:
            at = base + first * quarter
            src, dst, peer = rows(out_ref, at, quarter), rows(out_ref, at, quarter), peer_one
        else:
            src, dst, peer = rows(out_ref, base, half), rows(out_ref, base, half), mate
        return pltpu.make_async_remote_copy(
            src_ref=src, dst_ref=dst, send_sem=send_sem.at[chunk, phase], recv_sem=recv_sem.at[chunk, phase],
            device_id=(peer,), device_id_type=pl.DeviceIdType.MESH)

    def absorb(chunk, phase):
        base = chunk * size + core * half
        if phase == 0:
            at = pl.ds(pl.multiple_of(base, 8), half)
            buf_ref[at, :] = buf_ref[at, :] + in0_ref[chunk]
        elif phase == 1:
            at = pl.ds(pl.multiple_of(base + first * quarter, 8), quarter)
            buf_ref[at, :] = buf_ref[at, :] + in1_ref[chunk]
        elif phase == 2:
            at = pl.ds(pl.multiple_of(base + first * quarter + second * eighth, 8), eighth)
            out_ref[at, :] = buf_ref[at, :] + in2_ref[chunk]

    copies = {}
    for tick in range(6 + CHUNKS):
        for chunk in range(CHUNKS):
            phase = tick - chunk
            if phase >= 1 and phase <= 6:
                copies[chunk, phase - 1].wait_recv()
                absorb(chunk, phase - 1)
            if phase >= 0 and phase <= 5:
                copies[chunk, phase] = copy(chunk, phase)
                copies[chunk, phase].start()
    for done in copies.values():
        done.wait_send()


def sum_devices(low, mid, top_rows):
    n = low.shape[0] + mid.shape[0] + top_rows.shape[0] - 4
    vmem = pl.BlockSpec(memory_space=pltpu.VMEM)
    size = n // CHUNKS
    return pl.pallas_call(
        sum_kernel,
        in_specs=[vmem] * 3,
        out_specs=vmem,
        out_shape=jax.ShapeDtypeStruct((n, 128), F32),
        scratch_shapes=[pltpu.VMEM((n, 128), F32),
                        pltpu.VMEM((CHUNKS, size // 2, 128), F32),
                        pltpu.VMEM((CHUNKS, size // 4, 128), F32),
                        pltpu.VMEM((CHUNKS, size // 8, 128), F32),
                        pltpu.SemaphoreType.DMA((CHUNKS, 6)),
                        pltpu.SemaphoreType.DMA((CHUNKS, 6))],
        compiler_params=pltpu.CompilerParams(collective_id=1, has_side_effects=True, vmem_limit_bytes=VMEM_ALL),
        name="sum_devices",
    )(low, mid, top_rows)


def adam_update(params, adam_m, adam_v, grads):
    m_new = BETA_ONE * adam_m + (1.0 - BETA_ONE) * grads
    v_new = BETA_TWO * adam_v + (1.0 - BETA_TWO) * grads * grads
    m_hat = m_new / (1.0 - BETA_ONE ** STEP)
    v_hat = v_new / (1.0 - BETA_TWO ** STEP)
    return (params - ADAM_LR * m_hat / (jnp.sqrt(v_hat) + ADAM_EPS), m_new, v_new)


def stack_rows(*rows):
    width = HIDDEN
    rows = [jnp.pad(row, (0, width - row.shape[0])) for row in rows]
    rows += [jnp.zeros((width,), F32)] * (8 - len(rows))
    return jnp.stack(rows)


def solution(mesh):
    def body(feats, frontier, nbr_l1, mask_l1, nbr_l2, mask_l2, nbr_l3, mask_l3, labels, seed_mask, params, adam_m, adam_v):
        feat = feats.shape[1]
        classes = class_count(params.shape[0], feat)
        n_one = nbr_l1.shape[0]
        table = lax.all_gather(feats, 'dp', axis=0, tiled=True)
        pieces = unpack(params, feat, classes)
        pad3 = ((0, 0), (0, HIDDEN - classes))
        w3s = jnp.pad(pieces[10], pad3).astype(BF16)
        w3n = jnp.pad(pieces[11], pad3).astype(BF16)
        code_one = compose(frontier, nbr_l1.T, mask_l1.T)
        code_two = codes(nbr_l2.T, mask_l2.T, 256.0)
        m_one = count_matrix(code_one, table.shape[0])
        m_two = count_matrix(code_two, n_one)
        h_self, a_one, h_one, z_one_t = layer_one(
            m_one, code_one[2], table, frontier[:n_one], pieces[0].astype(BF16), pieces[1].astype(BF16),
            stack_rows(pieces[2], pieces[3], pieces[4]))
        a_two, h_two, z_two = layer_two(m_two, code_two[2], h_one, pieces[5].astype(BF16), pieces[6].astype(BF16),
                                        stack_rows(pieces[7], pieces[8], pieces[9]))
        g3s, g3n, mid_rows, vout, dself_t, dagg_t = top(
            classes, nbr_l3, mask_l3, labels[:, None], seed_mask[:, None], h_two, a_two, z_two, h_one, code_two[2],
            w3s, w3n, pieces[5].astype(BF16), pieces[6].astype(BF16),
            stack_rows(pieces[7], pieces[8], pieces[9], pieces[12]))
        gain_col = jnp.broadcast_to(pieces[3][:, None], (HIDDEN, 128))
        low_rows = bottom(dagg_t, m_two, dself_t, z_one_t, h_self, a_one, gain_col)
        n_params = params.shape[0]
        done = (low_rows.shape[0] + mid_rows.shape[0] - 4) * 128
        unit = 64 * CHUNKS * 128
        whole = -(-(n_params + 2) // unit) * unit
        top_rows = jnp.concatenate([g3s[:, :classes].reshape(-1), g3n[:, :classes].reshape(-1), vout[0, :classes],
                                    vout[1, :1], vout[2, :1],
                                    jnp.zeros((whole - n_params - 2,), F32)]).reshape((whole - done) // 128, 128)
        sums = sum_devices(low_rows, mid_rows, top_rows).reshape(-1)
        total = jnp.maximum(sums[n_params + 1], 1.0)
        loss = sums[n_params] / total
        return (loss,) + adam_update(params, adam_m, adam_v, sums[:n_params] / total)

    row_spec = P('dp')
    replicated = P()
    return jax.shard_map(body, mesh=mesh, in_specs=(row_spec,) * 10 + (replicated,) * 3,
                         out_specs=(replicated,) * 4, check_vma=False)
```

```python
import functools

import jax
import jax.numpy as jnp
from jax import lax
from jax.experimental import pallas as pl
from jax.experimental.pallas import tpu as pltpu
from jax.sharding import PartitionSpec as P

HIDDEN = 256
LANES = 128
WIDE = 256
GROUP = 16
SUB = 8
STEP = 10
LN_EPS = 1e-5
BETA_ONE = 0.9
BETA_TWO = 0.999
ADAM_LR = 3e-3
ADAM_EPS = 1e-8
F32 = jnp.float32
BF16 = jnp.bfloat16
F8 = jnp.float8_e4m3fn
VMEM_ALL = 60 * 1024 * 1024


def class_count(n_params, feat):
    return (n_params - 2 * feat * HIDDEN - 6 * HIDDEN - 2 * HIDDEN * HIDDEN) // (2 * HIDDEN + 1)


def params_of(*sem, vmem=VMEM_ALL):
    return pltpu.CompilerParams(dimension_semantics=sem, vmem_limit_bytes=vmem)


def emit_codes(lo, hi, mask, shift, low_ref, high_ref, count_ref):
    n = lo.shape[1]
    node = (lax.broadcasted_iota(jnp.int32, (GROUP, n), 1) & 15).astype(F32)
    code = jnp.where(mask > 0, hi * 16.0 + node - shift, -384.0)
    count = jnp.maximum(jnp.sum(mask, axis=0, keepdims=True), 1).astype(F32)
    mine = (lax.broadcasted_iota(jnp.int32, (SUB, LANES), 1) >> 4) == lax.broadcasted_iota(jnp.int32, (SUB, LANES), 0)
    fold = ((lax.broadcasted_iota(jnp.int32, (LANES, WIDE), 0) & 15)
            == (lax.broadcasted_iota(jnp.int32, (LANES, WIDE), 1) & 15)).astype(F32).astype(BF16)
    part = lax.broadcasted_iota(jnp.int32, (SUB, WIDE), 1) >> 4
    for c in range(n // LANES):
        lanes = slice(c * LANES, (c + 1) * LANES)
        count_ref[lanes, :] = jnp.broadcast_to(count[:, lanes], (LANES, LANES)).T
        for value, ref in ((lo, low_ref), (code, high_ref)):
            spread = jnp.concatenate([jnp.where(mine, jnp.broadcast_to(value[k:k + 1, lanes], (SUB, LANES)), 0.0)
                                      for k in range(GROUP)], axis=0)
            folded = jnp.dot(spread.astype(BF16), fold, preferred_element_type=F32)
            rows = folded[0:SUB, :]
            for k in range(1, GROUP):
                rows = jnp.where(part == k, folded[k * SUB:k * SUB + SUB, :], rows)
            ref[c * SUB:c * SUB + SUB, :] = rows


def pad_rows(x, rows):
    return jnp.concatenate([x, jnp.zeros((rows - x.shape[0], x.shape[1]), x.dtype)], axis=0)


def compose_kernel(front_ref, nbr_ref, mask_ref, low_ref, high_ref, count_ref, table_ref):
    fan, n = nbr_ref.shape

    @pl.when(pl.program_id(0) == 0)
    def _():
        ids = front_ref[...]
        table_ref[0:LANES, :] = (ids & 255).astype(F32).T.astype(BF16)
        table_ref[LANES:WIDE, :] = (ids >> SUB).astype(F32).T.astype(BF16)

    row = lax.broadcasted_iota(jnp.int32, (WIDE, n), 0).astype(F32).astype(BF16)
    one = jnp.ones((GROUP, n), BF16)
    zero = jnp.zeros((GROUP, n), BF16)
    sub = lax.broadcasted_iota(jnp.int32, (SUB, n), 0)
    lows, highs = [], []
    for k in range(fan):
        nbr = nbr_ref[k:k + 1, :]
        want = jnp.broadcast_to((nbr >> 7).astype(F32), (GROUP, n)).astype(BF16)
        pick = jnp.concatenate([jnp.where(row[p * GROUP:p * GROUP + GROUP, :] == want, one, zero) for p in range(GROUP)], axis=0)
        cand = jnp.dot(table_ref[...], pick, preferred_element_type=F32)
        lane = jnp.broadcast_to(nbr & 127, (SUB, n))
        low = jnp.zeros((SUB, n), F32)
        high = jnp.zeros((SUB, n), F32)
        for p in range(GROUP):
            hit = sub + p * SUB == lane
            low = jnp.where(hit, cand[p * SUB:p * SUB + SUB, :], low)
            high = jnp.where(hit, cand[LANES + p * SUB:136 + p * SUB, :], high)
        lows.append(jnp.sum(low, axis=0, keepdims=True))
        highs.append(jnp.sum(high, axis=0, keepdims=True))
    fill = [jnp.zeros((1, n), F32)] * (GROUP - fan)
    emit_codes(jnp.concatenate(lows + fill, axis=0), jnp.concatenate(highs + fill, axis=0),
               pad_rows(mask_ref[...], GROUP), 0.0, low_ref, high_ref, count_ref)


def codes_kernel(shift, nbr_ref, mask_ref, low_ref, high_ref, count_ref):
    ids = pad_rows(nbr_ref[...], GROUP)
    emit_codes((ids & 255).astype(F32), (ids >> SUB).astype(F32), pad_rows(mask_ref[...], GROUP), shift,
               low_ref, high_ref, count_ref)


def code_outs(n, block):
    rows = pl.BlockSpec((block // GROUP, WIDE), lambda i: (i, 0))
    shape = jax.ShapeDtypeStruct((n // GROUP, WIDE), F32)
    return dict(out_specs=[rows, rows, pl.BlockSpec((block, LANES), lambda i: (i, 0))],
                out_shape=[shape, shape, jax.ShapeDtypeStruct((n, LANES), F32)])


def compose(frontier, nbr_t, mask_t, block=512):
    fan, n = nbr_t.shape
    rows = frontier.shape[0] // LANES
    return pl.pallas_call(
        compose_kernel,
        grid=(n // block,),
        in_specs=[pl.BlockSpec((rows, LANES), lambda i: (0, 0)),
                  pl.BlockSpec((fan, block), lambda i: (0, i)),
                  pl.BlockSpec((fan, block), lambda i: (0, i))],
        **code_outs(n, block),
        scratch_shapes=[pltpu.VMEM((WIDE, rows), BF16)],
        compiler_params=params_of("arbitrary"),
        cost_estimate=pl.CostEstimate(flops=2 * 65536 * fan * n, bytes_accessed=10**7, transcendentals=0),
        name="compose_ids",
    )(frontier.reshape(rows, LANES), nbr_t, mask_t)


def codes(nbr_t, mask_t, shift, block=512):
    fan, n = nbr_t.shape
    return pl.pallas_call(
        functools.partial(codes_kernel, shift),
        grid=(n // block,),
        in_specs=[pl.BlockSpec((fan, block), lambda i: (0, i)),
                  pl.BlockSpec((fan, block), lambda i: (0, i))],
        **code_outs(n, block),
        compiler_params=params_of("arbitrary"),
        name="codes",
    )(nbr_t, mask_t)


def count_kernel(halves, unroll, low_ref, high_ref, out_ref):
    nodes = out_ref.shape[0]
    row = lax.broadcasted_iota(jnp.int32, (WIDE, WIDE), 0).astype(F32).astype(BF16)
    one = jnp.ones((GROUP, WIDE), BF16)
    zero = jnp.zeros((GROUP, WIDE), BF16)

    def one_hot(want, less):
        return [jnp.where(row[p * GROUP:p * GROUP + GROUP, :] - less == want, one, zero) for p in range(GROUP)]

    def group(g):
        at = pl.multiple_of(g * GROUP, GROUP)
        low = jnp.concatenate(one_hot(jnp.broadcast_to(low_ref[pl.ds(g, 1), :], (GROUP, WIDE)).astype(BF16), 0), axis=0)
        want = jnp.broadcast_to(high_ref[pl.ds(g, 1), :], (GROUP, WIDE)).astype(BF16)
        high = []
        for h in range(halves):
            high += one_hot(want, 0 if h == halves - 1 else WIDE)
        got = dot_t(jnp.concatenate(high, axis=0).astype(F8), low.astype(F8)).astype(BF16)
        for p in range(GROUP * halves):
            out_ref[pl.ds(at, GROUP), p * WIDE:(p + 1) * WIDE] = got[p * GROUP:p * GROUP + GROUP, :]

    def step(s, carry):
        for u in range(unroll):
            group(s * unroll + u)
        return carry

    lax.fori_loop(0, nodes // (GROUP * unroll), step, 0)


def count_matrix(code, vocab, block=WIDE, unroll=GROUP):
    low, high, _ = code
    n = low.shape[0] * GROUP
    rows = pl.BlockSpec((block // GROUP, WIDE), lambda i: (i, 0))
    return pl.pallas_call(
        functools.partial(count_kernel, vocab // 4096, unroll),
        grid=(n // block,),
        in_specs=[rows, rows],
        out_specs=pl.BlockSpec((block, vocab), lambda i: (i, 0)),
        out_shape=jax.ShapeDtypeStruct((n, vocab), BF16),
        compiler_params=params_of("arbitrary"),
        cost_estimate=pl.CostEstimate(flops=2 * n * vocab * WIDE, bytes_accessed=2 * n * vocab, transcendentals=0),
        name="count_matrix",
    )(low, high)


def norm_rows(z, gain, shift):
    act = jnp.maximum(z, 0.0)
    mean_act = jnp.mean(act, axis=-1, keepdims=True)
    centred = act - mean_act
    var_act = jnp.mean(centred * centred, axis=-1, keepdims=True)
    return centred * lax.rsqrt(var_act + LN_EPS) * gain + shift


def norm_back(z, gain, d_out, axis):
    act = jnp.maximum(z, 0.0)
    mean_act = jnp.mean(act, axis=axis, keepdims=True)
    centred = act - mean_act
    var_act = jnp.mean(centred * centred, axis=axis, keepdims=True)
    inv = lax.rsqrt(var_act + LN_EPS)
    hat = centred * inv
    d_hat = d_out * gain
    mean_d = jnp.mean(d_hat, axis=axis, keepdims=True)
    mean_dh = jnp.mean(d_hat * hat, axis=axis, keepdims=True)
    d_act = (d_hat - mean_d - hat * mean_dh) * inv
    return jnp.where(z > 0.0, d_act, 0.0), d_out * hat


def layer_one_kernel(self_ids, m_ref, codes_ref, *refs):
    part_refs = refs[:SUB]
    (w_self_ref, w_nbr_ref, vec_ref, hs_ref, a_ref, h_ref, zt_ref,
     x_ref, wide_ref, got_ref, hs_old_ref, a_old_ref, z_ref, sems) = refs[SUB:]
    block = m_ref.shape[0]
    rows, feat = x_ref.shape
    pid = pl.program_id(0)
    last = pl.num_programs(0) - 1
    tiles = feat // LANES

    @pl.when(pid == 0)
    def _():
        part = rows // SUB
        copies = [pltpu.make_async_copy(part_refs[p], x_ref.at[pl.ds(p * part, part), :], sems.at[p]) for p in range(SUB)]
        for copy in copies:
            copy.start()

        def spread(s, carry):
            at = pl.multiple_of(s * LANES, LANES)
            for c in range(tiles):
                wide_ref[pl.ds(at * SUB + c, LANES, stride=SUB), :] = x_ref[pl.ds(at, LANES), c * LANES:(c + 1) * LANES].astype(F32)
            return carry
        for p in range(SUB):
            copies[p].wait()
            lax.fori_loop(p * part // LANES, (p + 1) * part // LANES, spread, 0)
        hs_old_ref[...] = jnp.zeros_like(hs_old_ref)
        a_old_ref[...] = jnp.zeros_like(a_old_ref)

    def finish():
        z_ref[...] = (jnp.dot(hs_old_ref[...], w_self_ref[...], preferred_element_type=F32)
                      + jnp.dot(a_old_ref[...], w_nbr_ref[...], preferred_element_type=F32) + vec_ref[0:1, :])
        for at in range(0, block, LANES):
            z = z_ref[at:at + LANES, :]
            h_ref[at:at + LANES, :] = norm_rows(z, vec_ref[1:2, :], vec_ref[2:3, :]).astype(BF16)
            zt_ref[:, at:at + LANES] = z.T

    @pl.when(pid < last)
    def _():
        finish()
        for at in range(block):
            idx = self_ids[pid * block + at]
            got_ref[at * SUB:at * SUB + SUB, :] = wide_ref[pl.ds(pl.multiple_of(idx * SUB, SUB), SUB), :]
        share = 1.0 / codes_ref[:, 0:1]
        for c in range(feat // WIDE):
            cols = slice(c * WIDE, (c + 1) * WIDE)
            acc = jnp.dot(m_ref[...], x_ref[:, cols], preferred_element_type=F32)
            agg = (acc * share).astype(BF16)
            a_ref[:, cols] = agg
            a_old_ref[:, cols] = agg
        for c in range(tiles):
            piece = got_ref[pl.ds(c, block, stride=SUB), :].astype(BF16)
            hs_ref[:, c * LANES:(c + 1) * LANES] = piece
            hs_old_ref[:, c * LANES:(c + 1) * LANES] = piece

    @pl.when(pid == last)
    def _():
        finish()


def layer_one(m_one, code, parts, self_ids, w_self, w_nbr, vecs, block=512):
    n, rows = m_one.shape
    feat = parts[0].shape[1]
    steps = n // block
    whole = lambda i, ids: (0, 0)
    now = lambda i, ids: (jnp.minimum(i, steps - 1), 0)
    old = lambda i, ids: (jnp.maximum(i - 1, 0), 0)
    return pl.pallas_call(
        layer_one_kernel,
        grid_spec=pltpu.PrefetchScalarGridSpec(
            num_scalar_prefetch=1,
            grid=(steps + 1,),
            in_specs=[pl.BlockSpec((block, rows), now),
                      pl.BlockSpec((block, LANES), now)]
            + [pl.BlockSpec(memory_space=pl.ANY)] * SUB
            + [pl.BlockSpec((feat, HIDDEN), whole),
               pl.BlockSpec((feat, HIDDEN), whole),
               pl.BlockSpec((SUB, HIDDEN), whole)],
            out_specs=[pl.BlockSpec((block, feat), now),
                       pl.BlockSpec((block, feat), now),
                       pl.BlockSpec((block, HIDDEN), old),
                       pl.BlockSpec((HIDDEN, block), lambda i, ids: (0, jnp.maximum(i - 1, 0)))],
            scratch_shapes=[pltpu.VMEM((rows, feat), BF16), pltpu.VMEM((rows * SUB, LANES), F32),
                            pltpu.VMEM((block * SUB, LANES), F32), pltpu.VMEM((block, feat), BF16),
                            pltpu.VMEM((block, feat), BF16), pltpu.VMEM((block, HIDDEN), F32),
                            pltpu.SemaphoreType.DMA((SUB,))]),
        out_shape=[jax.ShapeDtypeStruct((n, feat), BF16),
                   jax.ShapeDtypeStruct((n, feat), BF16),
                   jax.ShapeDtypeStruct((n, HIDDEN), BF16),
                   jax.ShapeDtypeStruct((HIDDEN, n), F32)],
        compiler_params=params_of("arbitrary"),
        cost_estimate=pl.CostEstimate(flops=2 * n * rows * feat, bytes_accessed=2 * n * rows, transcendentals=0),
        name="layer_one",
    )(self_ids, m_one, code, *parts, w_self, w_nbr, vecs)


def layer_two_kernel(m_ref, codes_ref, h_all_ref, h_self_ref, w_self_ref, w_nbr_ref, vec_ref, a_ref, h_ref, z_ref):
    share = 1.0 / codes_ref[:, 0:1]
    acc = jnp.dot(m_ref[...], h_all_ref[...], preferred_element_type=F32)
    a_ref[...] = (acc * share).astype(BF16)
    z_ref[...] = (jnp.dot(h_self_ref[...], w_self_ref[...], preferred_element_type=F32)
                  + jnp.dot(a_ref[...], w_nbr_ref[...], preferred_element_type=F32) + vec_ref[0:1, :])
    for at in range(0, m_ref.shape[0], LANES):
        h_ref[at:at + LANES, :] = norm_rows(z_ref[at:at + LANES, :], vec_ref[1:2, :], vec_ref[2:3, :]).astype(BF16)


def layer_two(m_two, code, h_one, w_self, w_nbr, vecs, block=512):
    n, rows = m_two.shape
    whole = lambda i: (0, 0)
    by_row = lambda i: (i, 0)
    return pl.pallas_call(
        layer_two_kernel,
        grid=(n // block,),
        in_specs=[pl.BlockSpec((block, rows), by_row),
                  pl.BlockSpec((block, LANES), by_row),
                  pl.BlockSpec((rows, HIDDEN), whole),
                  pl.BlockSpec((block, HIDDEN), by_row),
                  pl.BlockSpec((HIDDEN, HIDDEN), whole),
                  pl.BlockSpec((HIDDEN, HIDDEN), whole),
                  pl.BlockSpec((SUB, HIDDEN), whole)],
        out_specs=[pl.BlockSpec((block, HIDDEN), by_row)] * 3,
        out_shape=[jax.ShapeDtypeStruct((n, HIDDEN), BF16),
                   jax.ShapeDtypeStruct((n, HIDDEN), BF16),
                   jax.ShapeDtypeStruct((n, HIDDEN), F32)],
        compiler_params=params_of("arbitrary"),
        cost_estimate=pl.CostEstimate(flops=2 * n * rows * HIDDEN, bytes_accessed=2 * n * rows, transcendentals=0),
        name="layer_two",
    )(m_two, code, h_one, h_one, w_self, w_nbr, vecs)


def tdot(lhs, rhs):
    return lax.dot_general(lhs, rhs, (((0,), (0,)), ((), ())), preferred_element_type=F32)


def dot_t(lhs, rhs):
    return lax.dot_general(lhs, rhs, (((1,), (1,)), ((), ())), preferred_element_type=F32)


def put_rows(ref, at, mat):
    n = mat.shape[0]
    ref[pl.ds(at, n, stride=2), :] = mat[:, 0:LANES]
    ref[pl.ds(at + 1, n, stride=2), :] = mat[:, LANES:WIDE]


def put_vector(ref, at, row):
    ref[at:at + 1, :] = row[:, 0:LANES]
    ref[at + 1:at + 2, :] = row[:, LANES:WIDE]


def top_kernel(classes, nbr3_ref, mask3_ref, label_ref, valid_ref, h2_ref, a2_ref, z2_ref, h1_ref, codes2_ref,
               w3s_ref, w3n_ref, w2s_ref, w2n_ref, vec_ref, bias3_ref,
               g3s_ref, g3n_ref, rows_ref, vout_ref, dself_ref, dagg_ref, m3_ref, dh2_ref, dz2_ref):
    fan, seeds = nbr3_ref.shape
    n_two = h2_ref.shape[0]
    piece = 512
    mask3 = mask3_ref[...]
    small = jnp.concatenate([jnp.where(mask3 > 0, nbr3_ref[...], -1), jnp.maximum(jnp.sum(mask3, axis=0, keepdims=True), 1),
                             label_ref[...], valid_ref[...], jnp.zeros((125 - fan, seeds), jnp.int32)], axis=0)
    small = jnp.concatenate([small[:, c * LANES:(c + 1) * LANES].T for c in range(seeds // LANES)], axis=0)
    count3 = small[:, fan:fan + 1].astype(F32)
    for c in range(n_two // piece):
        ids = lax.broadcasted_iota(jnp.int32, (seeds, piece), 1) + c * piece
        acc = jnp.zeros((seeds, piece), F32)
        for k in range(fan):
            acc = acc + jnp.where(ids == small[:, k:k + 1], 1.0, 0.0)
        m3_ref[:, c * piece:(c + 1) * piece] = acc.astype(BF16)
    a3 = (jnp.dot(m3_ref[...], h2_ref[...], preferred_element_type=F32) / count3).astype(BF16)
    self3 = h2_ref[0:seeds, :]
    logits = (jnp.dot(self3, w3s_ref[...], preferred_element_type=F32)
              + jnp.dot(a3, w3n_ref[...], preferred_element_type=F32) + bias3_ref[...])
    col = lax.broadcasted_iota(jnp.int32, logits.shape, 1)
    real = col < classes
    top = jnp.max(jnp.where(real, logits, -jnp.inf), axis=1, keepdims=True)
    powers = jnp.where(real, jnp.exp(logits - top), 0.0)
    total = jnp.sum(powers, axis=1, keepdims=True)
    log_norm = top + jnp.log(total)
    hot = col == small[:, fan + 1:fan + 2]
    picked = jnp.sum(jnp.where(hot, logits, 0.0), axis=1, keepdims=True)
    valid = small[:, fan + 2:fan + 3].astype(F32)
    loss = jnp.sum((log_norm - picked) * valid, axis=0, keepdims=True)
    n_valid = jnp.sum(valid, axis=0, keepdims=True)
    d_logits = (jnp.where(real, jnp.exp(logits - log_norm), 0.0) - jnp.where(hot, 1.0, 0.0)) * valid
    d_logb = d_logits.astype(BF16)
    g3s_ref[...] = tdot(self3, d_logb)
    g3n_ref[...] = tdot(a3, d_logb)
    d_self3 = dot_t(d_logb, w3s_ref[...])
    d_agg3 = (dot_t(d_logb, w3n_ref[...]) / count3).astype(BF16)
    dh2_ref[...] = tdot(m3_ref[...], d_agg3)
    dh2_ref[0:seeds, :] += d_self3
    sums = [jnp.zeros((1, HIDDEN), F32) for _ in range(3)]
    for at in range(0, n_two, LANES):
        span = slice(at, at + LANES)
        d_h2 = dh2_ref[span, :]
        d_z2, gain_terms = norm_back(z2_ref[span, :], vec_ref[1:2, :], d_h2, -1)
        dz2_ref[span, :] = d_z2.astype(BF16)
        for index, term in enumerate((d_z2, gain_terms, d_h2)):
            sums[index] = sums[index] + jnp.sum(term, axis=0, keepdims=True)
    d_bias = jnp.sum(d_logits, axis=0, keepdims=True)
    lane = lax.broadcasted_iota(jnp.int32, (1, LANES), 1)
    rest = classes - LANES
    tail = jnp.where(lane < rest, d_bias[:, LANES:WIDE],
                     jnp.where(lane == rest, loss, jnp.where(lane == rest + 1, n_valid, 0.0)))
    vout_ref[...] = jnp.concatenate([d_bias[:, 0:LANES], tail, jnp.zeros((6, LANES), F32)], axis=0)
    d_z2b = dz2_ref[...]
    put_rows(rows_ref, 0, tdot(h1_ref[...], d_z2b))
    put_rows(rows_ref, 2 * HIDDEN, tdot(a2_ref[...], d_z2b))
    for index in range(3):
        put_vector(rows_ref, 4 * HIDDEN + 2 * index, sums[index])
    rows_ref[4 * HIDDEN + 6:4 * HIDDEN + SUB, :] = jnp.zeros((2, LANES), F32)
    dself_ref[...] = dot_t(d_z2b, w2s_ref[...]).T
    count2 = codes2_ref[:, 0:1]
    dagg_ref[...] = (dot_t(d_z2b, w2n_ref[...]) / count2).T.astype(BF16)


def top(classes, nbr3, mask3, label, valid, h2, a2, z2, h1, codes2, w3s, w3n, w2s, w2n, vecs, bias3):
    n_two = h2.shape[0]
    seeds = nbr3.shape[1]
    square = jax.ShapeDtypeStruct((HIDDEN, HIDDEN), F32)
    rows = jax.ShapeDtypeStruct((4 * HIDDEN + SUB, LANES), F32)
    full = lambda x: pl.BlockSpec(x.shape, lambda i: (0, 0))
    args = (nbr3, mask3, label, valid, h2, a2, z2, h1, codes2, w3s, w3n, w2s, w2n, vecs, bias3)
    outs = [square, square, rows, jax.ShapeDtypeStruct((SUB, LANES), F32),
            jax.ShapeDtypeStruct((HIDDEN, n_two), F32), jax.ShapeDtypeStruct((HIDDEN, n_two), BF16)]
    specs = [full(x) for x in args]
    specs[7] = pl.BlockSpec((n_two, HIDDEN), lambda i: (0, 0))
    return pl.pallas_call(
        functools.partial(top_kernel, classes),
        grid=(1,),
        in_specs=specs,
        out_specs=[full(x) for x in outs],
        out_shape=outs,
        scratch_shapes=[pltpu.VMEM((seeds, n_two), BF16), pltpu.VMEM((n_two, HIDDEN), F32),
                        pltpu.VMEM((n_two, HIDDEN), BF16)],
        compiler_params=params_of("arbitrary"),
        name="layer_three",
    )(*args)


def bottom_kernel(dagg_ref, m_ref, dself_ref, zt_ref, hs_ref, a_ref, gain_ref, rows_ref,
                  gs_ref, gn_ref, vec_ref, dz_ref, dh_ref):
    pid = pl.program_id(0)
    last = pl.num_programs(0) - 1
    block = m_ref.shape[1]
    feat = hs_ref.shape[1]
    n_self = dself_ref.shape[1] // block

    @pl.when(pid == 0)
    def _():
        gs_ref[...] = jnp.zeros_like(gs_ref)
        gn_ref[...] = jnp.zeros_like(gn_ref)
        vec_ref[...] = jnp.zeros_like(vec_ref)
        dz_ref[...] = jnp.zeros_like(dz_ref)

    def weights():
        gs_ref[...] += jnp.dot(dz_ref[...], hs_ref[...], preferred_element_type=F32)
        gn_ref[...] += jnp.dot(dz_ref[...], a_ref[...], preferred_element_type=F32)

    @pl.when(pid < last)
    def _():
        weights()
        dh_ref[...] = jnp.dot(dagg_ref[...], m_ref[...], preferred_element_type=F32)

        @pl.when(pid < n_self)
        def _():
            dh_ref[...] += dself_ref[:, pl.ds(pl.multiple_of(pid * block, block), block)]

        for at in range(0, block, LANES):
            span = slice(at, at + LANES)
            d_h = dh_ref[:, span]
            d_z, gain_terms = norm_back(zt_ref[:, span], gain_ref[:, 0:1], d_h, 0)
            dz_ref[:, span] = d_z.astype(BF16)
            for index, term in enumerate((d_z, gain_terms, d_h)):
                vec_ref[index] += term

    @pl.when(pid == last)
    def _():
        weights()
        put_rows(rows_ref, 0, gs_ref[...].T)
        put_rows(rows_ref, 2 * feat, gn_ref[...].T)
        for index in range(3):
            put_vector(rows_ref, 4 * feat + 2 * index, jnp.sum(vec_ref[index].T, axis=0, keepdims=True))
        rows_ref[4 * feat + 6:4 * feat + SUB, :] = jnp.zeros((2, LANES), F32)


def bottom(dagg_t, m_two, dself_t, z_t, h_self, a_one, gain_col, block=1024):
    n_two, n = m_two.shape
    feat = h_self.shape[1]
    whole = lambda i: (0, 0)
    rows = 4 * feat + SUB
    steps = n // block
    now = lambda i: (0, jnp.minimum(i, steps - 1))
    old = lambda i: (jnp.maximum(i - 1, 0), 0)
    return pl.pallas_call(
        bottom_kernel,
        grid=(steps + 1,),
        in_specs=[pl.BlockSpec((HIDDEN, n_two), whole),
                  pl.BlockSpec((n_two, block), now),
                  pl.BlockSpec((HIDDEN, n_two), whole),
                  pl.BlockSpec((HIDDEN, block), now),
                  pl.BlockSpec((block, feat), old),
                  pl.BlockSpec((block, feat), old),
                  pl.BlockSpec((HIDDEN, LANES), whole)],
        out_specs=pl.BlockSpec((rows, LANES), whole),
        out_shape=jax.ShapeDtypeStruct((rows, LANES), F32),
        scratch_shapes=[pltpu.VMEM((HIDDEN, feat), F32), pltpu.VMEM((HIDDEN, feat), F32), pltpu.VMEM((3, HIDDEN, LANES), F32),
                        pltpu.VMEM((HIDDEN, block), BF16), pltpu.VMEM((HIDDEN, block), F32)],
        compiler_params=params_of("arbitrary"),
        cost_estimate=pl.CostEstimate(flops=2 * n * n_two * HIDDEN, bytes_accessed=2 * n * n_two, transcendentals=0),
        name="layer_one_back",
    )(dagg_t, m_two, dself_t, z_t, h_self, a_one, gain_col)


CHUNKS = 2
PHASES = 5


def sum_kernel(low_ref, mid_ref, top_ref, next_ref, tail_ref, out_ref, buf_ref, in0_ref, in1_ref, in2_ref, send_sem, recv_sem):
    me = lax.axis_index('dp')
    core = me % 2
    x_bit = (me // 2) % 2
    y_bit = me // 4
    x_peer = me + 2 - 4 * x_bit
    y_peer = me + 4 - SUB * y_bit
    mate = me + 1 - 2 * core
    first = x_bit + core * (y_bit - x_bit)
    peer_one = x_peer + core * (y_peer - x_peer)
    peer_two = y_peer + core * (x_peer - y_peer)
    barrier = pltpu.get_barrier_semaphore()
    for peer in (mate, x_peer, y_peer):
        pl.semaphore_signal(barrier, inc=1, device_id=(peer,), device_id_type=pl.DeviceIdType.MESH)
    at = 0
    for ref, count in ((low_ref, low_ref.shape[0] - 2), (mid_ref, mid_ref.shape[0] - 2),
                       (top_ref, top_ref.shape[0]), (next_ref, next_ref.shape[0]), (tail_ref, SUB)):
        buf_ref[at:at + count, :] = ref[0:count, :]
        at += count
    if at < buf_ref.shape[0]:
        buf_ref[at:, :] = jnp.zeros((buf_ref.shape[0] - at, LANES), F32)
    pl.semaphore_wait(barrier, 3)

    size = buf_ref.shape[0] // CHUNKS
    half, quarter = size // 2, size // 4

    def rows(ref, at, count):
        return ref.at[pl.ds(pl.multiple_of(at, SUB), count), :]

    def copy(chunk, phase):
        base = chunk * size + core * half
        if phase == 0:
            src, dst, peer = rows(buf_ref, chunk * size + (1 - core) * half, half), in0_ref.at[chunk], mate
        elif phase == 1:
            src, dst, peer = rows(buf_ref, base + (1 - first) * quarter, quarter), in1_ref.at[chunk], peer_one
        elif phase == 2:
            src, dst, peer = rows(buf_ref, base + first * quarter, quarter), in2_ref.at[chunk], peer_two
        elif phase == 3:
            at = base + first * quarter
            src, dst, peer = rows(out_ref, at, quarter), rows(out_ref, at, quarter), peer_one
        else:
            src, dst, peer = rows(out_ref, base, half), rows(out_ref, base, half), mate
        return pltpu.make_async_remote_copy(
            src_ref=src, dst_ref=dst, send_sem=send_sem.at[chunk, phase], recv_sem=recv_sem.at[chunk, phase],
            device_id=(peer,), device_id_type=pl.DeviceIdType.MESH)

    def absorb(chunk, phase):
        base = chunk * size + core * half
        if phase == 0:
            at = pl.ds(pl.multiple_of(base, SUB), half)
            buf_ref[at, :] = buf_ref[at, :] + in0_ref[chunk]
        elif phase == 1:
            at = pl.ds(pl.multiple_of(base + first * quarter, SUB), quarter)
            buf_ref[at, :] = buf_ref[at, :] + in1_ref[chunk]
        elif phase == 2:
            at = pl.ds(pl.multiple_of(base + first * quarter, SUB), quarter)
            out_ref[at, :] = buf_ref[at, :] + in2_ref[chunk]

    copies = {}
    for tick in range(PHASES + CHUNKS):
        for chunk in range(CHUNKS):
            phase = tick - chunk
            if 0 < phase <= PHASES:
                copies[chunk, phase - 1].wait_recv()
                absorb(chunk, phase - 1)
            if 0 <= phase < PHASES:
                copies[chunk, phase] = copy(chunk, phase)
                copies[chunk, phase].start()
    for done in copies.values():
        done.wait_send()


def sum_devices(*pieces):
    used = sum(piece.shape[0] for piece in pieces) - 4
    unit = 32 * CHUNKS
    n = -(-used // unit) * unit
    vmem = pl.BlockSpec(memory_space=pltpu.VMEM)
    size = n // CHUNKS
    return pl.pallas_call(
        sum_kernel,
        in_specs=[vmem] * 5,
        out_specs=vmem,
        out_shape=jax.ShapeDtypeStruct((n, LANES), F32),
        scratch_shapes=[pltpu.VMEM((n, LANES), F32),
                        pltpu.VMEM((CHUNKS, size // 2, LANES), F32),
                        pltpu.VMEM((CHUNKS, size // 4, LANES), F32),
                        pltpu.VMEM((CHUNKS, size // 4, LANES), F32),
                        pltpu.SemaphoreType.DMA((CHUNKS, PHASES)),
                        pltpu.SemaphoreType.DMA((CHUNKS, PHASES))],
        compiler_params=pltpu.CompilerParams(collective_id=1, has_side_effects=True, vmem_limit_bytes=VMEM_ALL),
        name="sum_devices",
    )(*pieces)


def adam_update(params, adam_m, adam_v, grads):
    m_new = BETA_ONE * adam_m + (1.0 - BETA_ONE) * grads
    v_new = BETA_TWO * adam_v + (1.0 - BETA_TWO) * grads * grads
    m_hat = m_new / (1.0 - BETA_ONE ** STEP)
    v_hat = v_new / (1.0 - BETA_TWO ** STEP)
    return (params - ADAM_LR * m_hat / (jnp.sqrt(v_hat) + ADAM_EPS), m_new, v_new)


def swap(x, bit):
    return lax.ppermute(x, 'dp', [(i, i ^ bit) for i in range(SUB)])


def weights_kernel(rows_ref, s1_ref, n1_ref, s2_ref, n2_ref, vec_ref, gain_ref):
    at = 0
    for ref in (s1_ref, n1_ref, None, s2_ref, n2_ref):
        if ref is None:
            at += 6
            continue
        n = ref.shape[0]
        ref[:, 0:LANES] = rows_ref[pl.ds(at, n, stride=2), :].astype(BF16)
        ref[:, LANES:WIDE] = rows_ref[pl.ds(at + 1, n, stride=2), :].astype(BF16)
        at += 2 * n
    feat = s1_ref.shape[0]
    for layer, base in enumerate((4 * feat, at)):
        for index in range(3):
            row = jnp.concatenate([rows_ref[base + 2 * index:base + 2 * index + 1, :],
                                   rows_ref[base + 2 * index + 1:base + 2 * index + 2, :]], axis=1)
            vec_ref[layer * SUB + index:layer * SUB + index + 1, :] = row
        vec_ref[layer * SUB + 3:layer * SUB + SUB, :] = jnp.zeros((5, HIDDEN), F32)
    gain_ref[...] = jnp.broadcast_to(vec_ref[1:2, :], (LANES, HIDDEN)).T


def weights(rows, feat):
    wide = jax.ShapeDtypeStruct((feat, HIDDEN), BF16)
    square = jax.ShapeDtypeStruct((HIDDEN, HIDDEN), BF16)
    vmem = pl.BlockSpec(memory_space=pltpu.VMEM)
    return pl.pallas_call(
        weights_kernel,
        in_specs=[vmem],
        out_specs=[vmem] * 6,
        out_shape=[wide, wide, square, square, jax.ShapeDtypeStruct((GROUP, HIDDEN), F32),
                   jax.ShapeDtypeStruct((HIDDEN, LANES), F32)],
        compiler_params=pltpu.CompilerParams(vmem_limit_bytes=VMEM_ALL),
        name="weights",
    )(rows)


def solution(mesh):
    def body(feats, frontier, nbr_l1, mask_l1, nbr_l2, mask_l2, nbr_l3, mask_l3, labels, seed_mask, params, adam_m, adam_v):
        feat = feats.shape[1]
        classes = class_count(params.shape[0], feat)
        n_one = nbr_l1.shape[0]
        rows_dev = feats.shape[0]
        groups = mesh.shape['dp']
        by_x = swap(feats, 2)
        by_y = swap(feats, 4)
        front = frontier ^ (lax.axis_index('dp') * rows_dev)
        used = (4 * feat + 4 * HIDDEN + 12) * LANES
        ws1, wn1, ws2, wn2, vecs, gain_col = weights(params[:used].reshape(-1, LANES), feat)
        span = HIDDEN * classes
        pad3 = ((0, 0), (0, HIDDEN - classes))
        w3s = jnp.pad(params[used:used + span].reshape(HIDDEN, classes).astype(BF16), pad3)
        w3n = jnp.pad(params[used + span:used + 2 * span].reshape(HIDDEN, classes).astype(BF16), pad3)
        bias3 = jnp.pad(params[used + 2 * span:].reshape(1, classes), ((0, 0), (0, HIDDEN - classes)))
        code_one = compose(front, nbr_l1.T, mask_l1.T)
        code_two = codes(nbr_l2.T, mask_l2.T, 256.0)
        code_one, by_x, by_y = lax.optimization_barrier((code_one, by_x, by_y))
        by_xy = swap(by_x, 4)
        m_one = count_matrix(code_one, groups * rows_dev)
        code_two, by_xy, m_one = lax.optimization_barrier((code_two, by_xy, m_one))
        parts = []
        for part in (feats, by_x, by_y, by_xy):
            parts += [part, swap(part, 1)]
        m_two = count_matrix(code_two, n_one)
        h_self, a_one, h_one, z_one_t = layer_one(m_one, code_one[2], parts, front[:n_one], ws1, wn1, vecs[:SUB])
        a_two, h_two, z_two = layer_two(m_two, code_two[2], h_one, ws2, wn2, vecs[SUB:])
        g3s, g3n, mid_rows, vout, dself_t, dagg_t = top(
            classes, nbr_l3.T, mask_l3.T, labels[None, :], seed_mask[None, :], h_two, a_two, z_two, h_one, code_two[2],
            w3s, w3n, ws2, wn2, vecs[SUB:], bias3)
        low_rows = bottom(dagg_t, m_two, dself_t, z_one_t, h_self, a_one, gain_col)
        n_params = params.shape[0]
        flat3 = [g[:, :classes].reshape(-1).reshape(-1, LANES) for g in (g3s, g3n)]
        sums = sum_devices(low_rows, mid_rows, *flat3, vout).reshape(-1)
        total = jnp.maximum(sums[n_params + 1], 1.0)
        loss = sums[n_params] / total
        return (loss,) + adam_update(params, adam_m, adam_v, sums[:n_params] / total)

    row_spec = P('dp')
    replicated = P()
    return jax.shard_map(body, mesh=mesh, in_specs=(row_spec,) * 10 + (replicated,) * 3,
                         out_specs=(replicated,) * 4, check_vma=False)
```

```python
import functools

import jax
import jax.numpy as jnp
from jax import lax
from jax.experimental import pallas as pl
from jax.experimental.pallas import tpu as pltpu
from jax.sharding import PartitionSpec as P

HIDDEN = 256
LANES = 128
WIDE = 256
GROUP = 16
SUB = 8
STEP = 10
LN_EPS = 1e-5
BETA_ONE = 0.9
BETA_TWO = 0.999
ADAM_LR = 3e-3
ADAM_EPS = 1e-8
F32 = jnp.float32
BF16 = jnp.bfloat16
F8 = jnp.float8_e4m3fn
VMEM_ALL = 60 * 1024 * 1024


def class_count(n_params, feat):
    return (n_params - 2 * feat * HIDDEN - 6 * HIDDEN - 2 * HIDDEN * HIDDEN) // (2 * HIDDEN + 1)


def params_of(*sem, vmem=VMEM_ALL):
    return pltpu.CompilerParams(dimension_semantics=sem, vmem_limit_bytes=vmem)


def emit_codes(lo, hi, mask, shift, low_ref, high_ref, count_ref):
    n = lo.shape[1]
    node = (lax.broadcasted_iota(jnp.int32, (GROUP, n), 1) & 15).astype(F32)
    code = jnp.where(mask > 0, hi * 16.0 + node - shift, -384.0)
    count = jnp.maximum(jnp.sum(mask, axis=0, keepdims=True), 1).astype(F32)
    mine = (lax.broadcasted_iota(jnp.int32, (SUB, LANES), 1) >> 4) == lax.broadcasted_iota(jnp.int32, (SUB, LANES), 0)
    fold = ((lax.broadcasted_iota(jnp.int32, (LANES, WIDE), 0) & 15)
            == (lax.broadcasted_iota(jnp.int32, (LANES, WIDE), 1) & 15)).astype(F32).astype(BF16)
    part = lax.broadcasted_iota(jnp.int32, (SUB, WIDE), 1) >> 4
    for c in range(n // LANES):
        lanes = slice(c * LANES, (c + 1) * LANES)
        count_ref[lanes, :] = jnp.broadcast_to(count[:, lanes], (LANES, LANES)).T
        for value, ref in ((lo, low_ref), (code, high_ref)):
            spread = jnp.concatenate([jnp.where(mine, jnp.broadcast_to(value[k:k + 1, lanes], (SUB, LANES)), 0.0)
                                      for k in range(GROUP)], axis=0)
            folded = jnp.dot(spread.astype(BF16), fold, preferred_element_type=F32)
            rows = folded[0:SUB, :]
            for k in range(1, GROUP):
                rows = jnp.where(part == k, folded[k * SUB:k * SUB + SUB, :], rows)
            ref[c * SUB:c * SUB + SUB, :] = rows


def pad_rows(x, rows):
    return jnp.concatenate([x, jnp.zeros((rows - x.shape[0], x.shape[1]), x.dtype)], axis=0)


def compose_kernel(front_ref, nbr_ref, mask_ref, low_ref, high_ref, count_ref, table_ref):
    fan, n = nbr_ref.shape

    @pl.when(pl.program_id(0) == 0)
    def _():
        ids = front_ref[...]
        table_ref[0:LANES, :] = (ids & 255).astype(F32).T.astype(BF16)
        table_ref[LANES:WIDE, :] = (ids >> SUB).astype(F32).T.astype(BF16)

    row = lax.broadcasted_iota(jnp.int32, (WIDE, n), 0).astype(F32).astype(BF16)
    one = jnp.ones((GROUP, n), BF16)
    zero = jnp.zeros((GROUP, n), BF16)
    sub = lax.broadcasted_iota(jnp.int32, (SUB, n), 0)
    lows, highs = [], []
    for k in range(fan):
        nbr = nbr_ref[k:k + 1, :]
        want = jnp.broadcast_to((nbr >> 7).astype(F32), (GROUP, n)).astype(BF16)
        pick = jnp.concatenate([jnp.where(row[p * GROUP:p * GROUP + GROUP, :] == want, one, zero) for p in range(GROUP)], axis=0)
        cand = jnp.dot(table_ref[...], pick, preferred_element_type=F32)
        lane = jnp.broadcast_to(nbr & 127, (SUB, n))
        low = jnp.zeros((SUB, n), F32)
        high = jnp.zeros((SUB, n), F32)
        for p in range(GROUP):
            hit = sub + p * SUB == lane
            low = jnp.where(hit, cand[p * SUB:p * SUB + SUB, :], low)
            high = jnp.where(hit, cand[LANES + p * SUB:136 + p * SUB, :], high)
        lows.append(jnp.sum(low, axis=0, keepdims=True))
        highs.append(jnp.sum(high, axis=0, keepdims=True))
    fill = [jnp.zeros((1, n), F32)] * (GROUP - fan)
    emit_codes(jnp.concatenate(lows + fill, axis=0), jnp.concatenate(highs + fill, axis=0),
               pad_rows(mask_ref[...], GROUP), 0.0, low_ref, high_ref, count_ref)


def codes_kernel(shift, nbr_ref, mask_ref, low_ref, high_ref, count_ref):
    ids = pad_rows(nbr_ref[...], GROUP)
    emit_codes((ids & 255).astype(F32), (ids >> SUB).astype(F32), pad_rows(mask_ref[...], GROUP), shift,
               low_ref, high_ref, count_ref)


def code_outs(n, block):
    rows = pl.BlockSpec((block // GROUP, WIDE), lambda i: (i, 0))
    shape = jax.ShapeDtypeStruct((n // GROUP, WIDE), F32)
    return dict(out_specs=[rows, rows, pl.BlockSpec((block, LANES), lambda i: (i, 0))],
                out_shape=[shape, shape, jax.ShapeDtypeStruct((n, LANES), F32)])


def compose(frontier, nbr_t, mask_t, block=2048):
    fan, n = nbr_t.shape
    rows = frontier.shape[0] // LANES
    return pl.pallas_call(
        compose_kernel,
        grid=(n // block,),
        in_specs=[pl.BlockSpec((rows, LANES), lambda i: (0, 0)),
                  pl.BlockSpec((fan, block), lambda i: (0, i)),
                  pl.BlockSpec((fan, block), lambda i: (0, i))],
        **code_outs(n, block),
        scratch_shapes=[pltpu.VMEM((WIDE, rows), BF16)],
        compiler_params=params_of("arbitrary"),
        cost_estimate=pl.CostEstimate(flops=2 * 65536 * fan * n, bytes_accessed=10**7, transcendentals=0),
        name="compose_ids",
    )(frontier.reshape(rows, LANES), nbr_t, mask_t)


def codes(nbr_t, mask_t, shift, block=1024):
    fan, n = nbr_t.shape
    return pl.pallas_call(
        functools.partial(codes_kernel, shift),
        grid=(n // block,),
        in_specs=[pl.BlockSpec((fan, block), lambda i: (0, i)),
                  pl.BlockSpec((fan, block), lambda i: (0, i))],
        **code_outs(n, block),
        compiler_params=params_of("arbitrary"),
        name="codes",
    )(nbr_t, mask_t)


def count_kernel(halves, unroll, low_ref, high_ref, out_ref):
    nodes = out_ref.shape[0]
    row = lax.broadcasted_iota(jnp.int32, (WIDE, WIDE), 0).astype(F32).astype(BF16)
    one = jnp.ones((GROUP, WIDE), BF16)
    zero = jnp.zeros((GROUP, WIDE), BF16)

    def one_hot(want, less):
        return [jnp.where(row[p * GROUP:p * GROUP + GROUP, :] - less == want, one, zero) for p in range(GROUP)]

    def group(g):
        at = pl.multiple_of(g * GROUP, GROUP)
        low = jnp.concatenate(one_hot(jnp.broadcast_to(low_ref[pl.ds(g, 1), :], (GROUP, WIDE)).astype(BF16), 0), axis=0)
        want = jnp.broadcast_to(high_ref[pl.ds(g, 1), :], (GROUP, WIDE)).astype(BF16)
        high = []
        for h in range(halves):
            high += one_hot(want, 0 if h == halves - 1 else WIDE)
        got = dot_t(jnp.concatenate(high, axis=0).astype(F8), low.astype(F8)).astype(BF16)
        for p in range(GROUP * halves):
            out_ref[pl.ds(at, GROUP), p * WIDE:(p + 1) * WIDE] = got[p * GROUP:p * GROUP + GROUP, :]

    def step(s, carry):
        for u in range(unroll):
            group(s * unroll + u)
        return carry

    lax.fori_loop(0, nodes // (GROUP * unroll), step, 0)


def count_matrix(code, vocab, block=512, unroll=32):
    low, high, _ = code
    n = low.shape[0] * GROUP
    rows = pl.BlockSpec((block // GROUP, WIDE), lambda i: (i, 0))
    return pl.pallas_call(
        functools.partial(count_kernel, vocab // 4096, unroll),
        grid=(n // block,),
        in_specs=[rows, rows],
        out_specs=pl.BlockSpec((block, vocab), lambda i: (i, 0)),
        out_shape=jax.ShapeDtypeStruct((n, vocab), BF16),
        compiler_params=params_of("arbitrary"),
        cost_estimate=pl.CostEstimate(flops=2 * n * vocab * WIDE, bytes_accessed=2 * n * vocab, transcendentals=0),
        name="count_matrix",
    )(low, high)


def norm_rows(z, gain, shift):
    act = jnp.maximum(z, 0.0)
    mean_act = jnp.mean(act, axis=-1, keepdims=True)
    centred = act - mean_act
    var_act = jnp.mean(centred * centred, axis=-1, keepdims=True)
    return centred * lax.rsqrt(var_act + LN_EPS) * gain + shift


def norm_back(z, gain, d_out, axis):
    act = jnp.maximum(z, 0.0)
    mean_act = jnp.mean(act, axis=axis, keepdims=True)
    centred = act - mean_act
    var_act = jnp.mean(centred * centred, axis=axis, keepdims=True)
    inv = lax.rsqrt(var_act + LN_EPS)
    hat = centred * inv
    d_hat = d_out * gain
    mean_d = jnp.mean(d_hat, axis=axis, keepdims=True)
    mean_dh = jnp.mean(d_hat * hat, axis=axis, keepdims=True)
    d_act = (d_hat - mean_d - hat * mean_dh) * inv
    return jnp.where(z > 0.0, d_act, 0.0), d_out * hat


def layer_one_kernel(self_ids, m_ref, codes_ref, *refs):
    part_refs = refs[:SUB]
    (w_self_ref, w_nbr_ref, vec_ref, hs_ref, a_ref, h_ref, zt_ref,
     x_ref, wide_ref, got_ref, hs_old_ref, a_old_ref, z_ref, sems) = refs[SUB:]
    block = m_ref.shape[0]
    rows, feat = x_ref.shape
    pid = pl.program_id(0)
    last = pl.num_programs(0) - 1
    tiles = feat // LANES

    @pl.when(pid == 0)
    def _():
        part = rows // SUB
        copies = [pltpu.make_async_copy(part_refs[p], x_ref.at[pl.ds(p * part, part), :], sems.at[p]) for p in range(SUB)]
        for copy in copies:
            copy.start()

        def spread(s, carry):
            at = pl.multiple_of(s * LANES, LANES)
            for c in range(tiles):
                wide_ref[pl.ds(at * SUB + c, LANES, stride=SUB), :] = x_ref[pl.ds(at, LANES), c * LANES:(c + 1) * LANES].astype(F32)
            return carry
        for p in range(SUB):
            copies[p].wait()
            lax.fori_loop(p * part // LANES, (p + 1) * part // LANES, spread, 0)
        hs_old_ref[...] = jnp.zeros_like(hs_old_ref)
        a_old_ref[...] = jnp.zeros_like(a_old_ref)

    def finish():
        z_ref[...] = (jnp.dot(hs_old_ref[...], w_self_ref[...], preferred_element_type=F32)
                      + jnp.dot(a_old_ref[...], w_nbr_ref[...], preferred_element_type=F32) + vec_ref[0:1, :])
        for at in range(0, block, LANES):
            z = z_ref[at:at + LANES, :]
            h_ref[at:at + LANES, :] = norm_rows(z, vec_ref[1:2, :], vec_ref[2:3, :]).astype(BF16)
            zt_ref[:, at:at + LANES] = z.T

    @pl.when(pid < last)
    def _():
        finish()
        for at in range(block):
            idx = self_ids[pid * block + at]
            got_ref[at * SUB:at * SUB + SUB, :] = wide_ref[pl.ds(pl.multiple_of(idx * SUB, SUB), SUB), :]
        share = 1.0 / codes_ref[:, 0:1]
        for c in range(feat // WIDE):
            cols = slice(c * WIDE, (c + 1) * WIDE)
            acc = jnp.dot(m_ref[...], x_ref[:, cols], preferred_element_type=F32)
            agg = (acc * share).astype(BF16)
            a_ref[:, cols] = agg
            a_old_ref[:, cols] = agg
        for c in range(tiles):
            piece = got_ref[pl.ds(c, block, stride=SUB), :].astype(BF16)
            hs_ref[:, c * LANES:(c + 1) * LANES] = piece
            hs_old_ref[:, c * LANES:(c + 1) * LANES] = piece

    @pl.when(pid == last)
    def _():
        finish()


def layer_one(m_one, code, parts, self_ids, w_self, w_nbr, vecs, block=512):
    n, rows = m_one.shape
    feat = parts[0].shape[1]
    steps = n // block
    whole = lambda i, ids: (0, 0)
    now = lambda i, ids: (jnp.minimum(i, steps - 1), 0)
    old = lambda i, ids: (jnp.maximum(i - 1, 0), 0)
    return pl.pallas_call(
        layer_one_kernel,
        grid_spec=pltpu.PrefetchScalarGridSpec(
            num_scalar_prefetch=1,
            grid=(steps + 1,),
            in_specs=[pl.BlockSpec((block, rows), now),
                      pl.BlockSpec((block, LANES), now)]
            + [pl.BlockSpec(memory_space=pl.ANY)] * SUB
            + [pl.BlockSpec((feat, HIDDEN), whole),
               pl.BlockSpec((feat, HIDDEN), whole),
               pl.BlockSpec((SUB, HIDDEN), whole)],
            out_specs=[pl.BlockSpec((block, feat), now),
                       pl.BlockSpec((block, feat), now),
                       pl.BlockSpec((block, HIDDEN), old),
                       pl.BlockSpec((HIDDEN, block), lambda i, ids: (0, jnp.maximum(i - 1, 0)))],
            scratch_shapes=[pltpu.VMEM((rows, feat), BF16), pltpu.VMEM((rows * SUB, LANES), F32),
                            pltpu.VMEM((block * SUB, LANES), F32), pltpu.VMEM((block, feat), BF16),
                            pltpu.VMEM((block, feat), BF16), pltpu.VMEM((block, HIDDEN), F32),
                            pltpu.SemaphoreType.DMA((SUB,))]),
        out_shape=[jax.ShapeDtypeStruct((n, feat), BF16),
                   jax.ShapeDtypeStruct((n, feat), BF16),
                   jax.ShapeDtypeStruct((n, HIDDEN), BF16),
                   jax.ShapeDtypeStruct((HIDDEN, n), F32)],
        compiler_params=params_of("arbitrary"),
        cost_estimate=pl.CostEstimate(flops=2 * n * rows * feat, bytes_accessed=2 * n * rows, transcendentals=0),
        name="layer_one",
    )(self_ids, m_one, code, *parts, w_self, w_nbr, vecs)


def layer_two_kernel(m_ref, codes_ref, h_all_ref, h_self_ref, w_self_ref, w_nbr_ref, vec_ref, a_ref, h_ref, z_ref):
    share = 1.0 / codes_ref[:, 0:1]
    acc = jnp.dot(m_ref[...], h_all_ref[...], preferred_element_type=F32)
    a_ref[...] = (acc * share).astype(BF16)
    z_ref[...] = (jnp.dot(h_self_ref[...], w_self_ref[...], preferred_element_type=F32)
                  + jnp.dot(a_ref[...], w_nbr_ref[...], preferred_element_type=F32) + vec_ref[0:1, :])
    for at in range(0, m_ref.shape[0], LANES):
        h_ref[at:at + LANES, :] = norm_rows(z_ref[at:at + LANES, :], vec_ref[1:2, :], vec_ref[2:3, :]).astype(BF16)


def layer_two(m_two, code, h_one, w_self, w_nbr, vecs, block=512):
    n, rows = m_two.shape
    whole = lambda i: (0, 0)
    by_row = lambda i: (i, 0)
    return pl.pallas_call(
        layer_two_kernel,
        grid=(n // block,),
        in_specs=[pl.BlockSpec((block, rows), by_row),
                  pl.BlockSpec((block, LANES), by_row),
                  pl.BlockSpec((rows, HIDDEN), whole),
                  pl.BlockSpec((block, HIDDEN), by_row),
                  pl.BlockSpec((HIDDEN, HIDDEN), whole),
                  pl.BlockSpec((HIDDEN, HIDDEN), whole),
                  pl.BlockSpec((SUB, HIDDEN), whole)],
        out_specs=[pl.BlockSpec((block, HIDDEN), by_row)] * 3,
        out_shape=[jax.ShapeDtypeStruct((n, HIDDEN), BF16),
                   jax.ShapeDtypeStruct((n, HIDDEN), BF16),
                   jax.ShapeDtypeStruct((n, HIDDEN), F32)],
        compiler_params=params_of("arbitrary"),
        cost_estimate=pl.CostEstimate(flops=2 * n * rows * HIDDEN, bytes_accessed=2 * n * rows, transcendentals=0),
        name="layer_two",
    )(m_two, code, h_one, h_one, w_self, w_nbr, vecs)


def tdot(lhs, rhs):
    return lax.dot_general(lhs, rhs, (((0,), (0,)), ((), ())), preferred_element_type=F32)


def dot_t(lhs, rhs):
    return lax.dot_general(lhs, rhs, (((1,), (1,)), ((), ())), preferred_element_type=F32)


def put_rows(ref, at, mat):
    n = mat.shape[0]
    ref[pl.ds(at, n, stride=2), :] = mat[:, 0:LANES]
    ref[pl.ds(at + 1, n, stride=2), :] = mat[:, LANES:WIDE]


def put_vector(ref, at, row):
    ref[at:at + 1, :] = row[:, 0:LANES]
    ref[at + 1:at + 2, :] = row[:, LANES:WIDE]


def top_kernel(classes, nbr3_ref, mask3_ref, label_ref, valid_ref, h2_ref, a2_ref, z2_ref, h1_ref, codes2_ref,
               w3s_ref, w3n_ref, w2s_ref, w2n_ref, vec_ref, bias3_ref,
               g3s_ref, g3n_ref, rows_ref, vout_ref, dself_ref, dagg_ref, m3_ref, dh2_ref, dz2_ref):
    fan, seeds = nbr3_ref.shape
    n_two = h2_ref.shape[0]
    piece = 512
    mask3 = mask3_ref[...]
    small = jnp.concatenate([jnp.where(mask3 > 0, nbr3_ref[...], -1), jnp.maximum(jnp.sum(mask3, axis=0, keepdims=True), 1),
                             label_ref[...], valid_ref[...], jnp.zeros((125 - fan, seeds), jnp.int32)], axis=0)
    small = jnp.concatenate([small[:, c * LANES:(c + 1) * LANES].T for c in range(seeds // LANES)], axis=0)
    count3 = small[:, fan:fan + 1].astype(F32)
    for c in range(n_two // piece):
        ids = lax.broadcasted_iota(jnp.int32, (seeds, piece), 1) + c * piece
        acc = jnp.zeros((seeds, piece), F32)
        for k in range(fan):
            acc = acc + jnp.where(ids == small[:, k:k + 1], 1.0, 0.0)
        m3_ref[:, c * piece:(c + 1) * piece] = acc.astype(BF16)
    a3 = (jnp.dot(m3_ref[...], h2_ref[...], preferred_element_type=F32) / count3).astype(BF16)
    self3 = h2_ref[0:seeds, :]
    logits = (jnp.dot(self3, w3s_ref[...], preferred_element_type=F32)
              + jnp.dot(a3, w3n_ref[...], preferred_element_type=F32) + bias3_ref[...])
    col = lax.broadcasted_iota(jnp.int32, logits.shape, 1)
    real = col < classes
    top = jnp.max(jnp.where(real, logits, -jnp.inf), axis=1, keepdims=True)
    powers = jnp.where(real, jnp.exp(logits - top), 0.0)
    total = jnp.sum(powers, axis=1, keepdims=True)
    log_norm = top + jnp.log(total)
    hot = col == small[:, fan + 1:fan + 2]
    picked = jnp.sum(jnp.where(hot, logits, 0.0), axis=1, keepdims=True)
    valid = small[:, fan + 2:fan + 3].astype(F32)
    loss = jnp.sum((log_norm - picked) * valid, axis=0, keepdims=True)
    n_valid = jnp.sum(valid, axis=0, keepdims=True)
    d_logits = (jnp.where(real, jnp.exp(logits - log_norm), 0.0) - jnp.where(hot, 1.0, 0.0)) * valid
    d_logb = d_logits.astype(BF16)
    g3s_ref[...] = tdot(self3, d_logb)
    g3n_ref[...] = tdot(a3, d_logb)
    d_self3 = dot_t(d_logb, w3s_ref[...])
    d_agg3 = (dot_t(d_logb, w3n_ref[...]) / count3).astype(BF16)
    dh2_ref[...] = tdot(m3_ref[...], d_agg3)
    dh2_ref[0:seeds, :] += d_self3
    sums = [jnp.zeros((1, HIDDEN), F32) for _ in range(3)]
    for at in range(0, n_two, LANES):
        span = slice(at, at + LANES)
        d_h2 = dh2_ref[span, :]
        d_z2, gain_terms = norm_back(z2_ref[span, :], vec_ref[1:2, :], d_h2, -1)
        dz2_ref[span, :] = d_z2.astype(BF16)
        for index, term in enumerate((d_z2, gain_terms, d_h2)):
            sums[index] = sums[index] + jnp.sum(term, axis=0, keepdims=True)
    d_bias = jnp.sum(d_logits, axis=0, keepdims=True)
    lane = lax.broadcasted_iota(jnp.int32, (1, LANES), 1)
    rest = classes - LANES
    tail = jnp.where(lane < rest, d_bias[:, LANES:WIDE],
                     jnp.where(lane == rest, loss, jnp.where(lane == rest + 1, n_valid, 0.0)))
    vout_ref[...] = jnp.concatenate([d_bias[:, 0:LANES], tail, jnp.zeros((6, LANES), F32)], axis=0)
    d_z2b = dz2_ref[...]
    put_rows(rows_ref, 0, tdot(h1_ref[...], d_z2b))
    put_rows(rows_ref, 2 * HIDDEN, tdot(a2_ref[...], d_z2b))
    for index in range(3):
        put_vector(rows_ref, 4 * HIDDEN + 2 * index, sums[index])
    rows_ref[4 * HIDDEN + 6:4 * HIDDEN + SUB, :] = jnp.zeros((2, LANES), F32)
    dself_ref[...] = dot_t(d_z2b, w2s_ref[...]).T
    count2 = codes2_ref[:, 0:1]
    dagg_ref[...] = (dot_t(d_z2b, w2n_ref[...]) / count2).T.astype(BF16)


def top(classes, nbr3, mask3, label, valid, h2, a2, z2, h1, codes2, w3s, w3n, w2s, w2n, vecs, bias3):
    n_two = h2.shape[0]
    seeds = nbr3.shape[1]
    square = jax.ShapeDtypeStruct((HIDDEN, HIDDEN), F32)
    rows = jax.ShapeDtypeStruct((4 * HIDDEN + SUB, LANES), F32)
    full = lambda x: pl.BlockSpec(x.shape, lambda i: (0, 0))
    args = (nbr3, mask3, label, valid, h2, a2, z2, h1, codes2, w3s, w3n, w2s, w2n, vecs, bias3)
    outs = [square, square, rows, jax.ShapeDtypeStruct((SUB, LANES), F32),
            jax.ShapeDtypeStruct((HIDDEN, n_two), F32), jax.ShapeDtypeStruct((HIDDEN, n_two), BF16)]
    specs = [full(x) for x in args]
    specs[7] = pl.BlockSpec((n_two, HIDDEN), lambda i: (0, 0))
    return pl.pallas_call(
        functools.partial(top_kernel, classes),
        grid=(1,),
        in_specs=specs,
        out_specs=[full(x) for x in outs],
        out_shape=outs,
        scratch_shapes=[pltpu.VMEM((seeds, n_two), BF16), pltpu.VMEM((n_two, HIDDEN), F32),
                        pltpu.VMEM((n_two, HIDDEN), BF16)],
        compiler_params=params_of("arbitrary"),
        name="layer_three",
    )(*args)


def bottom_kernel(dagg_ref, m_ref, dself_ref, zt_ref, hs_ref, a_ref, gain_ref, rows_ref,
                  gs_ref, gn_ref, vec_ref, dz_ref, dh_ref):
    pid = pl.program_id(0)
    last = pl.num_programs(0) - 1
    block = m_ref.shape[1]
    feat = hs_ref.shape[1]
    n_self = dself_ref.shape[1] // block

    @pl.when(pid == 0)
    def _():
        gs_ref[...] = jnp.zeros_like(gs_ref)
        gn_ref[...] = jnp.zeros_like(gn_ref)
        vec_ref[...] = jnp.zeros_like(vec_ref)
        dz_ref[...] = jnp.zeros_like(dz_ref)

    def weights():
        gs_ref[...] += jnp.dot(dz_ref[...], hs_ref[...], preferred_element_type=F32)
        gn_ref[...] += jnp.dot(dz_ref[...], a_ref[...], preferred_element_type=F32)

    @pl.when(pid < last)
    def _():
        weights()
        dh_ref[...] = jnp.dot(dagg_ref[...], m_ref[...], preferred_element_type=F32)

        @pl.when(pid < n_self)
        def _():
            dh_ref[...] += dself_ref[:, pl.ds(pl.multiple_of(pid * block, block), block)]

        for at in range(0, block, LANES):
            span = slice(at, at + LANES)
            d_h = dh_ref[:, span]
            d_z, gain_terms = norm_back(zt_ref[:, span], gain_ref[:, 0:1], d_h, 0)
            dz_ref[:, span] = d_z.astype(BF16)
            for index, term in enumerate((d_z, gain_terms, d_h)):
                vec_ref[index] += term

    @pl.when(pid == last)
    def _():
        weights()
        put_rows(rows_ref, 0, gs_ref[...].T)
        put_rows(rows_ref, 2 * feat, gn_ref[...].T)
        for index in range(3):
            put_vector(rows_ref, 4 * feat + 2 * index, jnp.sum(vec_ref[index].T, axis=0, keepdims=True))
        rows_ref[4 * feat + 6:4 * feat + SUB, :] = jnp.zeros((2, LANES), F32)


def bottom(dagg_t, m_two, dself_t, z_t, h_self, a_one, gain_col, block=1024):
    n_two, n = m_two.shape
    feat = h_self.shape[1]
    whole = lambda i: (0, 0)
    rows = 4 * feat + SUB
    steps = n // block
    now = lambda i: (0, jnp.minimum(i, steps - 1))
    old = lambda i: (jnp.maximum(i - 1, 0), 0)
    return pl.pallas_call(
        bottom_kernel,
        grid=(steps + 1,),
        in_specs=[pl.BlockSpec((HIDDEN, n_two), whole),
                  pl.BlockSpec((n_two, block), now),
                  pl.BlockSpec((HIDDEN, n_two), whole),
                  pl.BlockSpec((HIDDEN, block), now),
                  pl.BlockSpec((block, feat), old),
                  pl.BlockSpec((block, feat), old),
                  pl.BlockSpec((HIDDEN, LANES), whole)],
        out_specs=pl.BlockSpec((rows, LANES), whole),
        out_shape=jax.ShapeDtypeStruct((rows, LANES), F32),
        scratch_shapes=[pltpu.VMEM((HIDDEN, feat), F32), pltpu.VMEM((HIDDEN, feat), F32), pltpu.VMEM((3, HIDDEN, LANES), F32),
                        pltpu.VMEM((HIDDEN, block), BF16), pltpu.VMEM((HIDDEN, block), F32)],
        compiler_params=params_of("arbitrary"),
        cost_estimate=pl.CostEstimate(flops=2 * n * n_two * HIDDEN, bytes_accessed=2 * n * n_two, transcendentals=0),
        name="layer_one_back",
    )(dagg_t, m_two, dself_t, z_t, h_self, a_one, gain_col)


CHUNKS = 2
PHASES = 5


def sum_kernel(low_ref, mid_ref, top_ref, next_ref, tail_ref, out_ref, buf_ref, in0_ref, in1_ref, in2_ref, send_sem, recv_sem):
    me = lax.axis_index('dp')
    core = me % 2
    x_bit = (me // 2) % 2
    y_bit = me // 4
    x_peer = me + 2 - 4 * x_bit
    y_peer = me + 4 - SUB * y_bit
    mate = me + 1 - 2 * core
    first = x_bit + core * (y_bit - x_bit)
    peer_one = x_peer + core * (y_peer - x_peer)
    peer_two = y_peer + core * (x_peer - y_peer)
    barrier = pltpu.get_barrier_semaphore()
    for peer in (mate, x_peer, y_peer):
        pl.semaphore_signal(barrier, inc=1, device_id=(peer,), device_id_type=pl.DeviceIdType.MESH)
    at = 0
    for ref, count in ((low_ref, low_ref.shape[0] - 2), (mid_ref, mid_ref.shape[0] - 2),
                       (top_ref, top_ref.shape[0]), (next_ref, next_ref.shape[0]), (tail_ref, SUB)):
        buf_ref[at:at + count, :] = ref[0:count, :]
        at += count
    if at < buf_ref.shape[0]:
        buf_ref[at:, :] = jnp.zeros((buf_ref.shape[0] - at, LANES), F32)
    pl.semaphore_wait(barrier, 3)

    size = buf_ref.shape[0] // CHUNKS
    half, quarter = size // 2, size // 4

    def rows(ref, at, count):
        return ref.at[pl.ds(pl.multiple_of(at, SUB), count), :]

    def copy(chunk, phase):
        base = chunk * size + core * half
        if phase == 0:
            src, dst, peer = rows(buf_ref, chunk * size + (1 - core) * half, half), in0_ref.at[chunk], mate
        elif phase == 1:
            src, dst, peer = rows(buf_ref, base + (1 - first) * quarter, quarter), in1_ref.at[chunk], peer_one
        elif phase == 2:
            src, dst, peer = rows(buf_ref, base + first * quarter, quarter), in2_ref.at[chunk], peer_two
        elif phase == 3:
            at = base + first * quarter
            src, dst, peer = rows(out_ref, at, quarter), rows(out_ref, at, quarter), peer_one
        else:
            src, dst, peer = rows(out_ref, base, half), rows(out_ref, base, half), mate
        return pltpu.make_async_remote_copy(
            src_ref=src, dst_ref=dst, send_sem=send_sem.at[chunk, phase], recv_sem=recv_sem.at[chunk, phase],
            device_id=(peer,), device_id_type=pl.DeviceIdType.MESH)

    def absorb(chunk, phase):
        base = chunk * size + core * half
        if phase == 0:
            at = pl.ds(pl.multiple_of(base, SUB), half)
            buf_ref[at, :] = buf_ref[at, :] + in0_ref[chunk]
        elif phase == 1:
            at = pl.ds(pl.multiple_of(base + first * quarter, SUB), quarter)
            buf_ref[at, :] = buf_ref[at, :] + in1_ref[chunk]
        elif phase == 2:
            at = pl.ds(pl.multiple_of(base + first * quarter, SUB), quarter)
            out_ref[at, :] = buf_ref[at, :] + in2_ref[chunk]

    copies = {}
    for tick in range(PHASES + CHUNKS):
        for chunk in range(CHUNKS):
            phase = tick - chunk
            if 0 < phase <= PHASES:
                copies[chunk, phase - 1].wait_recv()
                absorb(chunk, phase - 1)
            if 0 <= phase < PHASES:
                copies[chunk, phase] = copy(chunk, phase)
                copies[chunk, phase].start()
    for done in copies.values():
        done.wait_send()


def sum_devices(*pieces):
    used = sum(piece.shape[0] for piece in pieces) - 4
    unit = 32 * CHUNKS
    n = -(-used // unit) * unit
    vmem = pl.BlockSpec(memory_space=pltpu.VMEM)
    size = n // CHUNKS
    return pl.pallas_call(
        sum_kernel,
        in_specs=[vmem] * 5,
        out_specs=vmem,
        out_shape=jax.ShapeDtypeStruct((n, LANES), F32),
        scratch_shapes=[pltpu.VMEM((n, LANES), F32),
                        pltpu.VMEM((CHUNKS, size // 2, LANES), F32),
                        pltpu.VMEM((CHUNKS, size // 4, LANES), F32),
                        pltpu.VMEM((CHUNKS, size // 4, LANES), F32),
                        pltpu.SemaphoreType.DMA((CHUNKS, PHASES)),
                        pltpu.SemaphoreType.DMA((CHUNKS, PHASES))],
        compiler_params=pltpu.CompilerParams(collective_id=1, has_side_effects=True, vmem_limit_bytes=VMEM_ALL),
        name="sum_devices",
    )(*pieces)


def adam_update(params, adam_m, adam_v, grads):
    m_new = BETA_ONE * adam_m + (1.0 - BETA_ONE) * grads
    v_new = BETA_TWO * adam_v + (1.0 - BETA_TWO) * grads * grads
    m_hat = m_new / (1.0 - BETA_ONE ** STEP)
    v_hat = v_new / (1.0 - BETA_TWO ** STEP)
    return (params - ADAM_LR * m_hat / (jnp.sqrt(v_hat) + ADAM_EPS), m_new, v_new)


def swap(x, bit):
    return lax.ppermute(x, 'dp', [(i, i ^ bit) for i in range(SUB)])


def weights_kernel(rows_ref, s1_ref, n1_ref, s2_ref, n2_ref, vec_ref, gain_ref):
    at = 0
    for ref in (s1_ref, n1_ref, None, s2_ref, n2_ref):
        if ref is None:
            at += 6
            continue
        n = ref.shape[0]
        ref[:, 0:LANES] = rows_ref[pl.ds(at, n, stride=2), :].astype(BF16)
        ref[:, LANES:WIDE] = rows_ref[pl.ds(at + 1, n, stride=2), :].astype(BF16)
        at += 2 * n
    feat = s1_ref.shape[0]
    for layer, base in enumerate((4 * feat, at)):
        for index in range(3):
            row = jnp.concatenate([rows_ref[base + 2 * index:base + 2 * index + 1, :],
                                   rows_ref[base + 2 * index + 1:base + 2 * index + 2, :]], axis=1)
            vec_ref[layer * SUB + index:layer * SUB + index + 1, :] = row
        vec_ref[layer * SUB + 3:layer * SUB + SUB, :] = jnp.zeros((5, HIDDEN), F32)
    gain_ref[...] = jnp.broadcast_to(vec_ref[1:2, :], (LANES, HIDDEN)).T


def weights(rows, feat):
    wide = jax.ShapeDtypeStruct((feat, HIDDEN), BF16)
    square = jax.ShapeDtypeStruct((HIDDEN, HIDDEN), BF16)
    vmem = pl.BlockSpec(memory_space=pltpu.VMEM)
    return pl.pallas_call(
        weights_kernel,
        in_specs=[vmem],
        out_specs=[vmem] * 6,
        out_shape=[wide, wide, square, square, jax.ShapeDtypeStruct((GROUP, HIDDEN), F32),
                   jax.ShapeDtypeStruct((HIDDEN, LANES), F32)],
        compiler_params=pltpu.CompilerParams(vmem_limit_bytes=VMEM_ALL),
        name="weights",
    )(rows)


def solution(mesh):
    def body(feats, frontier, nbr_l1, mask_l1, nbr_l2, mask_l2, nbr_l3, mask_l3, labels, seed_mask, params, adam_m, adam_v):
        feat = feats.shape[1]
        classes = class_count(params.shape[0], feat)
        n_one = nbr_l1.shape[0]
        rows_dev = feats.shape[0]
        groups = mesh.shape['dp']
        by_x = swap(feats, 2)
        by_y = swap(feats, 4)
        front = frontier ^ (lax.axis_index('dp') * rows_dev)
        used = (4 * feat + 4 * HIDDEN + 12) * LANES
        ws1, wn1, ws2, wn2, vecs, gain_col = weights(params[:used].reshape(-1, LANES), feat)
        span = HIDDEN * classes
        pad3 = ((0, 0), (0, HIDDEN - classes))
        w3s = jnp.pad(params[used:used + span].reshape(HIDDEN, classes).astype(BF16), pad3)
        w3n = jnp.pad(params[used + span:used + 2 * span].reshape(HIDDEN, classes).astype(BF16), pad3)
        bias3 = jnp.pad(params[used + 2 * span:].reshape(1, classes), ((0, 0), (0, HIDDEN - classes)))
        code_one = compose(front, nbr_l1.T, mask_l1.T)
        code_two = codes(nbr_l2.T, mask_l2.T, 256.0)
        code_one, by_x, by_y = lax.optimization_barrier((code_one, by_x, by_y))
        by_xy = swap(by_x, 4)
        m_one = count_matrix(code_one, groups * rows_dev, 1024, 64)
        code_two, by_xy, m_one = lax.optimization_barrier((code_two, by_xy, m_one))
        parts = []
        for part in (feats, by_x, by_y, by_xy):
            parts += [part, swap(part, 1)]
        m_two = count_matrix(code_two, n_one)
        h_self, a_one, h_one, z_one_t = layer_one(m_one, code_one[2], parts, front[:n_one], ws1, wn1, vecs[:SUB])
        a_two, h_two, z_two = layer_two(m_two, code_two[2], h_one, ws2, wn2, vecs[SUB:])
        g3s, g3n, mid_rows, vout, dself_t, dagg_t = top(
            classes, nbr_l3.T, mask_l3.T, labels[None, :], seed_mask[None, :], h_two, a_two, z_two, h_one, code_two[2],
            w3s, w3n, ws2, wn2, vecs[SUB:], bias3)
        low_rows = bottom(dagg_t, m_two, dself_t, z_one_t, h_self, a_one, gain_col)
        n_params = params.shape[0]
        flat3 = [g[:, :classes].reshape(-1).reshape(-1, LANES) for g in (g3s, g3n)]
        sums = sum_devices(low_rows, mid_rows, *flat3, vout).reshape(-1)
        total = jnp.maximum(sums[n_params + 1], 1.0)
        loss = sums[n_params] / total
        return (loss,) + adam_update(params, adam_m, adam_v, sums[:n_params] / total)

    row_spec = P('dp')
    replicated = P()
    return jax.shard_map(body, mesh=mesh, in_specs=(row_spec,) * 10 + (replicated,) * 3,
                         out_specs=(replicated,) * 4, check_vma=False)
```
